32 devices in a mesh: row: 4 (over z), col: 8 (over y, x, core).
Axes of the slice: x: 2, y: 2, z: 4, core: 2. Of those that a mesh axis runs over, the one named last changes fastest.
Arguments:
- tile_values: bfloat16 [4, 8, 128, 128, 128], P('row', 'col'), may hold values from -0.1875 to 0.1875
- tile_rows: int32 [4, 8, 128], P('row', 'col'), may hold values from 0 to 15, as said below
- tile_cols: int32 [4, 8, 128], P('row', 'col'), may hold values from 0 to 15, as said below
- tile_count: int32 [4, 8], P('row', 'col'), may hold values from 42 to 128, as said below
- sinogram: float32 [8192, 128], P('row'), may hold values from -6 to 6
Outputs:
- solution: float32 [16384, 128], P('col')
- residual_estimate: float32 [128], replicated
The draws below stay inside these ranges and needn't reach their ends.
Inputs may be any that keep to these rules, and one draw needn't show every extreme that they name: On each device the 128 slots name distinct tile positions (tile_rows, tile_cols) of its grid of 16 x 16 tiles. `tile_cols`: see tile_rows. `tile_count`: some device holds 128 tiles in every draw.
All inputs are finite; a program needn't handle non-finite values.
Results may differ from the reference program's by a relative error of at most 0.0019.
Values may be sent and summed in bfloat16 or wider, within the bound.
A program may use at most 128 MiB of HBM per device.

```python
import jax
import jax.numpy as jnp
from jax import lax

TILE = 128
TR = 16
TC = 16
CAP = 128
Z = 128
ITERS = 3
M = 8192
N_ROW = 4
N_COL = 8


def occupancy(key):
    base = jax.random.fold_in(key, 7)
    device_keys = jax.random.split(base, N_ROW * N_COL)
    orders = jax.vmap(lambda single: jax.random.permutation(single, TR * TC))(device_keys)
    return orders[:, :CAP].reshape(N_ROW, N_COL, CAP).astype(jnp.int32)


def draw_tile_rows(key, part):
    return (occupancy(key) // TC).astype(jnp.int32)


def draw_tile_cols(key, part):
    return (occupancy(key) % TC).astype(jnp.int32)


def draw_tile_count(key, part):
    counts = jax.random.randint(jax.random.fold_in(key, 11), (N_ROW * N_COL,), CAP // 3, CAP + 1)
    fullest = jax.random.randint(jax.random.fold_in(key, 13), (), 0, N_ROW * N_COL)
    flat = jnp.where(jnp.arange(N_ROW * N_COL) == fullest, CAP, counts)
    return flat.reshape(N_ROW, N_COL).astype(jnp.int32)


def steps_of(stream_key, shape, pieces, least, top_value):
    factor_of = 1.0
    for position, parts in pieces:
        steps = jax.random.uniform(jax.random.fold_in(jax.random.fold_in(stream_key, 6), position), (parts,), jnp.float32, least / len(pieces), top_value / len(pieces))
        factor_of = factor_of * jnp.repeat(jnp.exp(steps), shape[position] // parts).reshape((-1,) + (1,) * (len(shape) - 1 - position))
    return factor_of


def scatter_about(stream_key, extent, scale, limit, cuts=(), kind=jnp.bfloat16):
    entries = scale * jax.random.normal(stream_key, extent, jnp.float32)
    if cuts:
        entries = entries * steps_of(stream_key, extent, cuts, -0.22, 0.18)
    return jnp.clip(entries, -limit, limit).astype(kind)


def setup_inputs(seed: int = 0) -> dict:
    arg_keys = jax.random.split(jax.random.key(seed), 6)
    return {
        "tile_values": scatter_about(arg_keys[0], (N_ROW, N_COL, CAP, TILE, TILE), (TILE * CAP // TR) ** -0.5, 0.1875, ((0, 4), (1, 8))),
        "tile_rows": draw_tile_rows(jax.random.fold_in(arg_keys[5], 71), 0),
        "tile_cols": draw_tile_cols(jax.random.fold_in(arg_keys[5], 71), 0),
        "tile_count": draw_tile_count(jax.random.fold_in(arg_keys[5], 71), 0),
        "sinogram": scatter_about(arg_keys[4], (M, Z), 1.0, 6.0, ((0, 4),), jnp.float32),
    }


EPSILON = 1e-06

def column_norm(vec):
    return jnp.sqrt(lax.optimization_barrier(jnp.sum(vec * vec, axis=0)) + EPSILON)

def project(tile_values, tile_rows, tile_cols, tile_count, source, forward):
    operand = source.astype(jnp.bfloat16).astype(jnp.float32)
    slot_ids = jnp.arange(CAP, dtype=jnp.int32)
    if forward:
        out_rows = TR * TILE * N_ROW
        out_blocks = TR
        in_len = TC * TILE
        pattern = 'tij,tjz->tiz'
    else:
        out_rows = TC * TILE * N_COL
        out_blocks = TC
        in_len = TR * TILE
        pattern = 'tji,tjz->tiz'

    def one_device(carry, device_idx):
        row_idx = device_idx // N_COL
        col_idx = device_idx % N_COL
        values = tile_values[row_idx, col_idx].astype(jnp.float32)
        if forward:
            take_index = tile_cols[row_idx, col_idx]
            put_index = tile_rows[row_idx, col_idx]
            in_first = (col_idx * in_len).astype(jnp.int32)
            out_first = (row_idx * (out_blocks * TILE)).astype(jnp.int32)
        else:
            take_index = tile_rows[row_idx, col_idx]
            put_index = tile_cols[row_idx, col_idx]
            in_first = (row_idx * in_len).astype(jnp.int32)
            out_first = (col_idx * (out_blocks * TILE)).astype(jnp.int32)
        blocks = lax.dynamic_slice_in_dim(operand, in_first, in_len, 0).reshape(in_len // TILE, TILE, Z)
        products = jnp.einsum(pattern, values, blocks[take_index], precision=lax.Precision.HIGHEST)
        live_mask = (slot_ids < tile_count[row_idx, col_idx]).astype(jnp.float32)
        targets = jnp.arange(out_blocks, dtype=jnp.int32)
        onehot = (put_index[None, :] == targets[:, None]).astype(jnp.float32) * live_mask[None, :]
        part_sum = jnp.einsum('rt,tiz->riz', onehot, products, precision=lax.Precision.HIGHEST)
        part_sum = part_sum.reshape(out_blocks * TILE, Z)
        current = lax.dynamic_slice_in_dim(carry, out_first, out_blocks * TILE, 0)
        return (lax.dynamic_update_slice_in_dim(carry, current + part_sum, out_first, 0), None)
    start = jnp.zeros((out_rows, Z), jnp.float32)
    result, unused = lax.scan(one_device, start, jnp.arange(N_ROW * N_COL, dtype=jnp.int32))
    return result

def rotation(rho_bar, beta_norm, phi_bar):
    rho_value = jnp.sqrt(rho_bar * rho_bar + beta_norm * beta_norm)
    cosine = rho_bar / rho_value
    sine_value = beta_norm / rho_value
    return (rho_value, cosine, sine_value, cosine * phi_bar, sine_value * phi_bar)

def reference(tile_values, tile_rows, tile_cols, tile_count, sinogram):
    beta_norm = column_norm(sinogram)
    ray_vec = sinogram / beta_norm
    voxel_raw = project(tile_values, tile_rows, tile_cols, tile_count, sinogram, False) / beta_norm
    alpha_norm = column_norm(voxel_raw)
    voxel_vec = voxel_raw / alpha_norm
    search_dir = voxel_vec
    solution = jnp.zeros_like(voxel_vec)
    phi_bar = beta_norm
    rho_bar = alpha_norm
    for step_idx in range(ITERS):
        ray_raw = project(tile_values, tile_rows, tile_cols, tile_count, voxel_raw, True) / alpha_norm - alpha_norm * ray_vec
        beta_norm = column_norm(ray_raw)
        ray_vec = ray_raw / beta_norm
        rho_value, cosine, sine_value, phi_value, phi_bar = rotation(rho_bar, beta_norm, phi_bar)
        solution = solution + phi_value / rho_value * search_dir
        if step_idx + 1 < ITERS:
            voxel_raw = project(tile_values, tile_rows, tile_cols, tile_count, ray_raw, False) / beta_norm - beta_norm * voxel_vec
            alpha_norm = column_norm(voxel_raw)
            voxel_vec = voxel_raw / alpha_norm
            theta_value = sine_value * alpha_norm
            rho_bar = -cosine * alpha_norm
            search_dir = voxel_vec - theta_value / rho_value * search_dir
    return (solution, phi_bar)
```

```python
import functools

import jax
import jax.numpy as jnp
from jax import lax
from jax.experimental import pallas as pl
from jax.experimental.pallas import tpu as pltpu
from jax.sharding import PartitionSpec as P

TC = 16
ITERS = 3
EPSILON = 1e-06
PAD = 16
TOP = 32000.0
FINE = 64.0
LANE = 128
MESH = pl.DeviceIdType.MESH


def pack(val):
    top = jnp.max(jnp.abs(val), axis=0, keepdims=True)
    exponent = jnp.ceil(jnp.log2(jnp.maximum(top, 1e-30)))
    scale = TOP * jnp.exp2(-exponent)
    coded = jnp.round(jnp.clip(val * scale, -32767.0, 32767.0))
    coded = coded.astype(jnp.int32).astype(jnp.int16)
    rows = jnp.broadcast_to(exponent, (PAD, val.shape[1]))
    return coded, rows.astype(jnp.int32).astype(jnp.int16)


def store_packet(ref, val):
    n = val.shape[0]
    coded, rows = pack(val)
    ref[pl.ds(0, n), :] = coded
    ref[pl.ds(n, PAD), :] = rows


def load_packet(ref):
    n = ref.shape[0] - PAD
    exponent = ref[pl.ds(n, PAD), :].astype(jnp.int32).astype(jnp.float32)[:1]
    scale = jnp.exp2(exponent) * (1.0 / TOP)
    return ref[pl.ds(0, n), :].astype(jnp.int32).astype(jnp.float32) * scale


def dot(a, b):
    return jnp.dot(a, b, preferred_element_type=jnp.float32)


def root(total_of):
    return jnp.sqrt(total_of() + EPSILON)


def squares(vec):
    return jnp.sum(vec * vec, axis=0, keepdims=True)


def kernel_rows(
    nr, nc, inv, tiles, sino, sol, res,
    facc, bacc, sq, fa, ba, ybf, xbf, ray, vox, vfull, sdir,
    bsend, brecv, vgat, dsend, drecv, fsend, frecv, rgat, nrow, ncol, nlast,
    bs, br, vs, vr, ds_, dr, fs, fr, gs, gr, hs, hr, rs, rr, cs, cr, ls, lr,
):
    mr = lax.axis_index("row")
    mc = lax.axis_index("col")
    nch = nc // 2
    chip = mc // 2
    core = mc % 2
    partner = chip * 2 + (1 - core)
    tile = tiles.shape[1]
    mb, z = sino.shape
    nb = sol.shape[0]
    tr, tc = mb // tile, nb // tile
    sv, sr = nb // nr, mb // nc

    barrier = pltpu.get_barrier_semaphore()
    for s in range(1, nr):
        pl.semaphore_signal(barrier, 1, device_id=(lax.rem(mr + s, nr), mc), device_id_type=MESH)
    for s in range(1, nc):
        pl.semaphore_signal(barrier, 1, device_id=(mr, lax.rem(mc + s, nc)), device_id_type=MESH)

    def send(src, dst, ssem, rsem, row, col):
        copy = pltpu.make_async_remote_copy(
            src_ref=src, dst_ref=dst, send_sem=ssem, recv_sem=rsem,
            device_id=(row, col), device_id_type=MESH)
        copy.start()
        sent.append(copy)
        return copy

    sent = []

    def pick(i, j):
        slot = inv[i * tc + j]
        block = tiles[jnp.maximum(slot, 0)]
        return jnp.where(slot >= 0, block, jnp.zeros_like(block))

    @pl.loop(0, tc)
    def _(j):
        first = pl.multiple_of(j * tile, tile)
        for i in range(tr):
            ba[pl.ds(first, tile), i * tile:(i + 1) * tile] = pick(i, j).T

    def share(vec, buf, n, me, ssem, rsem, over_row):
        buf[me] = jnp.broadcast_to(vec, (8, z))
        copies = []
        for s in range(1, n):
            peer = lax.rem(me + s, n)
            place = (peer, mc) if over_row else (mr, peer)
            copies.append(send(buf.at[me], buf.at[me], ssem.at[s], rsem.at[s], *place))

        def finish():
            for copy in copies:
                copy.wait_recv()
            total = buf[0]
            for q in range(1, n):
                total = total + buf[q]
            return total[:1]

        return finish

    line = nr == 4
    inner = (mr == 1) | (mr == 2)
    left = mr < 2
    mate = mr + 1 - 2 * lax.rem(mr, 2)
    cross = jnp.where(left, 2, 1)
    far = jnp.where(left, 3, 0)
    early = jnp.where(inner, far, mate)
    late = jnp.where(inner, mate, far)
    inner_sent = []

    def row_copy(src, dst, ssem, rsem, row):
        return pltpu.make_async_remote_copy(
            src_ref=src, dst_ref=dst, send_sem=ssem, recv_sem=rsem,
            device_id=(row, mc), device_id_type=MESH)

    def back_part(k, dest):
        rows = pl.ds(pl.multiple_of(dest * sv, sv), sv)
        if k == 0:
            return dot(ba[rows, :], ybf[...])
        late = lax.rem(chip + 1, nch) * 2 * sr
        cols = pl.ds(pl.multiple_of(late, 2 * sr), 2 * sr)
        return bacc[rows, :] + dot(ba[rows, cols], ybf[cols, :])

    def back_arrived(k, slot):
        row_copy(bsend.at[k, slot], brecv.at[k, slot], bs.at[k, slot], br.at[k, slot], mate).wait_recv()

    def back_start(k):
        if line:
            store_packet(bsend.at[k, 0], back_part(k, jnp.where(inner, cross, far)))
            slot = jnp.where(inner, 3, 0)
            send(bsend.at[k, 0], brecv.at[k, slot], bs.at[k, 0], br.at[k, slot],
                 jnp.where(inner, cross, mate), mc)
            part = back_part(k, jnp.where(inner, far, cross))

            @pl.when(jnp.logical_not(inner))
            def _():
                store_packet(bsend.at[k, 1], part)

            @pl.when(inner)
            def _():
                back_arrived(k, 0)
                store_packet(bsend.at[k, 1], part + load_packet(brecv.at[k, 0]))

            send(bsend.at[k, 1], brecv.at[k, 1], bs.at[k, 1], br.at[k, 1], jnp.where(inner, far, cross), mc)
            store_packet(bsend.at[k, 2], back_part(k, mate))
            send(bsend.at[k, 2], brecv.at[k, 2], bs.at[k, 2], br.at[k, 2], mate, mc)
            vox[k] = back_part(k, mr)
            return None
        copies = []
        for s in list(range(1, nr)) + [0]:
            dest = lax.rem(mr + s, nr)
            part = back_part(k, dest)
            if s:
                store_packet(bsend.at[k, s], part)
                copies.append(send(bsend.at[k, s], brecv.at[k, s], bs.at[k, s], br.at[k, s], dest, mc))
            else:
                vox[k] = part
        return copies

    def back_sum(k, copies):
        if line:
            @pl.when(inner)
            def _():
                back_arrived(k, 3)
                vox[k] = vox[k] + load_packet(brecv.at[k, 3])

            total = vox[k]
            for slot in (2, 1):
                back_arrived(k, slot)
                total = total + load_packet(brecv.at[k, slot])
            return total
        total = vox[k]
        for i, copy in enumerate(copies):
            copy.wait_recv()
            total = total + load_packet(brecv.at[k, i + 1])
        return total

    def vox_take(k, origin):
        val = load_packet(vgat.at[k, origin])
        rows = pl.ds(pl.multiple_of(origin * sv, sv), sv)
        vfull[rows, :] = val
        xbf[rows, :] = val.astype(jnp.bfloat16)

    def grow(acc, mat, vec, first, depth, fresh):
        cols = pl.ds(pl.multiple_of(first, depth), depth)

        @pl.loop(0, acc.shape[0] // sv)
        def _(i):
            rows = pl.ds(pl.multiple_of(i * sv, sv), sv)
            val = dot(mat[rows, cols], vec[cols, :])
            acc[rows, :] = val if fresh else acc[rows, :] + val

    def vox_gather(k):
        store_packet(vgat.at[k, mr], vox[k])
        if line:
            def passed(origin, n, row):
                return row_copy(vgat.at[k, origin], vgat.at[k, origin], vs.at[k, n], vr.at[k, origin], row)

            @pl.when(inner)
            def _():
                passed(mr, 2, far).start()

            send(vgat.at[k, mr], vgat.at[k, mr], vs.at[k, 1], vr.at[k, mr], cross, mc)
            send(vgat.at[k, mr], vgat.at[k, mr], vs.at[k, 0], vr.at[k, mr], mate, mc)
            inner_sent.append(passed(mr, 2, far))
            inner_sent.append(passed(far, 3, mate))
            vox_take(k, mr)
            grow(facc, fa, xbf, mr * sv, sv, True)

            @pl.when(inner)
            def _():
                passed(far, 3, mate).wait_recv()
                passed(far, 3, mate).start()

            @pl.when(jnp.logical_not(inner))
            def _():
                passed(mate, 0, mate).wait_recv()

            vox_take(k, early)
            grow(facc, fa, xbf, early * sv, sv, False)
            passed(cross, 0, mate).wait_recv()
            vox_take(k, cross)
            grow(facc, fa, xbf, cross * sv, sv, False)
            passed(late, 0, mate).wait_recv()
            vox_take(k, late)
        else:
            copies = [
                send(vgat.at[k, mr], vgat.at[k, mr], vs.at[k, s], vr.at[k, s], lax.rem(mr + s, nr), mc)
                for s in range(1, nr)
            ]
            for copy in copies:
                copy.wait_recv()
            for q in range(nr):
                vox_take(k, q)
        return share(squares(vfull[...]), ncol.at[k], nc, mc, cs.at[k], cr.at[k], False)

    def fwd_part(first):
        rows = pl.ds(first, sr)
        if line:
            cols = pl.ds(pl.multiple_of(late * sv, sv), sv)
            return facc[rows, :] + dot(fa[rows, cols], xbf[cols, :])
        return dot(fa[rows, :], xbf[...])

    def fwd_start(k):
        order = list(range(1, nch)) + [0]
        local = []
        for s in order:
            q = lax.rem(chip + s, nch)
            first = pl.multiple_of((q * 2 + 1 - core) * sr, sr)
            dsend[k, s] = fwd_part(first)
            local.append(send(dsend.at[k, s], drecv.at[k, s], ds_.at[k, s], dr.at[k, s], mr, partner))
        copies = []
        for s, other in zip(order, local):
            q = lax.rem(chip + s, nch)
            first = pl.multiple_of((q * 2 + core) * sr, sr)
            part = fwd_part(first)
            other.wait_recv()
            part = part + drecv[k, s]
            if s:
                store_packet(fsend.at[k, s], part)
                copies.append(send(fsend.at[k, s], frecv.at[k, s], fs.at[k, s], fr.at[k, s], mr, q * 2 + core))
            else:
                ray[k + 1] = part
        return copies

    def fwd_sum(k, copies):
        total = ray[k + 1]
        for i, copy in enumerate(copies):
            copy.wait_recv()
            total = total + load_packet(frecv.at[k, i + 1])
        return total

    def ray_gather(k):
        store_packet(rgat.at[k, mc], ray[k + 1])
        across = [send(rgat.at[k, mc], rgat.at[k, mc], gs.at[k, 0], gr.at[k, 0], mr, partner)]
        for s in range(1, nch):
            peer = lax.rem(chip + s, nch) * 2 + core
            across.append(send(rgat.at[k, mc], rgat.at[k, mc], gs.at[k, s], gr.at[k, s], mr, peer))
        hand = [None]

        def take(origin):
            val = load_packet(rgat.at[k, origin])
            sq[origin] = jnp.broadcast_to(squares(val), (8, z))
            ybf[pl.ds(pl.multiple_of(origin * sr, sr), sr), :] = val.astype(jnp.bfloat16)

        take(mc)
        across[0].wait_recv()
        take(partner)
        grow(bacc, ba, ybf, chip * 2 * sr, 2 * sr, True)
        for s in range(1, nch):
            across[s].wait_recv()
            origin = lax.rem(chip + nch - s, nch) * 2 + core
            hand.append(send(rgat.at[k, origin], rgat.at[k, origin], hs.at[k, s], hr.at[k, s], mr, partner))
            take(origin)
        for s in range(1, nch):
            hand[s].wait_recv()
            origin = lax.rem(chip + nch - s, nch) * 2
            take(origin + 1 - core)
            if s + 1 < nch:
                grow(bacc, ba, ybf, origin * sr, 2 * sr, False)
        total = jnp.zeros((1, z), jnp.float32)
        for q in range(nc):
            total = total + sq[q][:1]
        return share(total, nrow.at[k + 1], nr, mr, rs.at[k + 1], rr.at[k + 1], True)

    ybf[...] = sino[...].astype(jnp.bfloat16)
    total = squares(sino[...])
    pl.semaphore_wait(barrier, nr - 1 + nc - 1)
    beta_of = share(total, nrow.at[0], nr, mr, rs.at[0], rr.at[0], True)
    copies = back_start(0)

    @pl.loop(0, tr)
    def _(i):
        first = pl.multiple_of(i * tile, tile)
        for j in range(tc):
            fa[pl.ds(first, tile), j * tile:(j + 1) * tile] = pick(i, j)

    beta = root(beta_of)
    ray[0] = sino[pl.ds(pl.multiple_of(mc * sr, sr), sr), :] * (1.0 / beta)
    vox[0] = back_sum(0, copies) * (1.0 / beta)
    alpha_of = vox_gather(0)
    phi_bar = beta
    for k in range(ITERS):
        copies = fwd_start(k)
        alpha = root(alpha_of)
        inv_alpha = 1.0 / alpha
        if k == 0:
            rho_bar = alpha
            sdir[...] = vfull[...] * inv_alpha
        else:
            theta = sine * alpha
            rho_bar = -cosine * alpha
            sdir[...] = vfull[...] * inv_alpha - (theta / rho) * sdir[...]
        vox[k] = vox[k] * inv_alpha
        ray_raw = fwd_sum(k, copies) * inv_alpha - alpha * ray[k]
        last = k + 1 == ITERS
        if last:
            total = share(squares(ray_raw), nlast, nc, mc, ls, lr, False)()
            beta = root(share(total, nrow.at[k + 1], nr, mr, rs.at[k + 1], rr.at[k + 1], True))
        else:
            ray[k + 1] = ray_raw
            beta_of = ray_gather(k)
            copies = back_start(k + 1)
            beta = root(beta_of)
            ray[k + 1] = ray[k + 1] * (1.0 / beta)
        rho = jnp.sqrt(rho_bar * rho_bar + beta * beta)
        cosine = rho_bar / rho
        sine = beta / rho
        phi = cosine * phi_bar
        phi_bar = sine * phi_bar
        step = (phi / rho) * sdir[...]
        sol[...] = step if k == 0 else sol[...] + step
        if not last:
            vox[k + 1] = back_sum(k + 1, copies) * (1.0 / beta) - beta * vox[k]
            alpha_of = vox_gather(k + 1)
    res[...] = jnp.broadcast_to(phi_bar, res.shape)
    for copy in sent:
        copy.wait_send()
    if line:
        @pl.when(inner)
        def _():
            for copy in inner_sent:
                copy.wait_send()


def body_rows(nr, nc, tile_values, tile_rows, tile_cols, tile_count, sinogram):
    values = tile_values[0, 0]
    slots, tile = values.shape[0], values.shape[1]
    mb, z = sinogram.shape
    nb = TC * tile
    tr = mb // tile
    place = tile_rows[0, 0] * TC + tile_cols[0, 0]
    ids = jnp.arange(slots, dtype=jnp.int32)
    place = jnp.where(ids < tile_count[0, 0], place, -1)
    hit = place[None, :] == jnp.arange(tr * TC, dtype=jnp.int32)[:, None]
    inv = jnp.sum(jnp.where(hit, ids[None, :] + 1, 0), axis=1, dtype=jnp.int32) - 1
    nch = nc // 2
    sv, sr = nb // nr, mb // nc
    f32, bf16, i16 = jnp.float32, jnp.bfloat16, jnp.int16
    dma = pltpu.SemaphoreType.DMA
    vmem = pl.BlockSpec(memory_space=pltpu.VMEM)
    scratch = [
        pltpu.VMEM((mb, z), f32), pltpu.VMEM((nb, z), f32), pltpu.VMEM((nc, 8, z), f32),
        pltpu.VMEM((mb, nb), bf16), pltpu.VMEM((nb, mb), bf16),
        pltpu.VMEM((mb, z), bf16), pltpu.VMEM((nb, z), bf16),
        pltpu.VMEM((ITERS + 1, sr, z), f32), pltpu.VMEM((ITERS, sv, z), f32),
        pltpu.VMEM((nb, z), f32), pltpu.VMEM((nb, z), f32),
        pltpu.VMEM((ITERS, nr, sv + PAD, z), i16), pltpu.VMEM((ITERS, nr, sv + PAD, z), i16),
        pltpu.VMEM((ITERS, nr, sv + PAD, z), i16),
        pltpu.VMEM((ITERS, nch, sr, z), f32), pltpu.VMEM((ITERS, nch, sr, z), f32),
        pltpu.VMEM((ITERS, nch, sr + PAD, z), i16), pltpu.VMEM((ITERS, nch, sr + PAD, z), i16),
        pltpu.VMEM((ITERS, nc, sr + PAD, z), i16),
        pltpu.VMEM((ITERS + 1, nr, 8, z), f32), pltpu.VMEM((ITERS, nc, 8, z), f32),
        pltpu.VMEM((nc, 8, z), f32),
        dma((ITERS, nr)), dma((ITERS, nr)), dma((ITERS, nr)), dma((ITERS, nr)),
        dma((ITERS, nch)), dma((ITERS, nch)), dma((ITERS, nch)), dma((ITERS, nch)),
        dma((ITERS, nch)), dma((ITERS, nch)), dma((ITERS, nch)), dma((ITERS, nch)),
        dma((ITERS + 1, nr)), dma((ITERS + 1, nr)), dma((ITERS, nc)), dma((ITERS, nc)),
        dma((nc,)), dma((nc,)),
    ]
    sol, res = pl.pallas_call(
        functools.partial(kernel_rows, nr, nc),
        out_shape=(jax.ShapeDtypeStruct((nb, z), f32), jax.ShapeDtypeStruct((8, z), f32)),
        in_specs=[pl.BlockSpec(memory_space=pltpu.SMEM), vmem, vmem],
        out_specs=(vmem, vmem),
        scratch_shapes=scratch,
        compiler_params=pltpu.CompilerParams(
            collective_id=0, has_side_effects=True, vmem_limit_bytes=60 * 1024 * 1024),
    )(inv, values, sinogram)
    return sol, res[0]


def col_pack(ref, val):
    h, n = val.shape
    groups = h // PAD
    mag = jnp.abs(val)
    top = mag[:PAD]
    for g in range(1, groups):
        top = jnp.maximum(top, mag[g * PAD:(g + 1) * PAD])
    top = jnp.max(top, axis=1, keepdims=True)
    exponent = jnp.ceil(jnp.log2(jnp.maximum(top, 1e-30)) * FINE)
    scale = jnp.concatenate([TOP * jnp.exp2(exponent * (-1.0 / FINE))] * groups, axis=0)
    coded = jnp.round(val * scale).astype(jnp.int32).astype(jnp.int16)
    for j in range(n // LANE):
        ref[pl.ds(j * h, h), :] = coded[:, j * LANE:(j + 1) * LANE]
    ref[pl.ds(n // LANE * h, PAD), :] = jnp.broadcast_to(exponent, (PAD, LANE)).astype(jnp.int32).astype(jnp.int16)


def col_unpack(ref, h):
    blocks = (ref.shape[0] - PAD) // h
    exponent = ref[pl.ds(blocks * h, PAD), :].astype(jnp.int32).astype(jnp.float32)
    scale = jnp.concatenate([jnp.exp2(exponent * (1.0 / FINE)) * (1.0 / TOP)] * (h // PAD), axis=0)
    return jnp.concatenate(
        [ref[pl.ds(j * h, h), :].astype(jnp.int32).astype(jnp.float32) * scale for j in range(blocks)], axis=1)


def row_squares(val):
    h, n = val.shape
    acc = jnp.zeros((h, LANE), jnp.float32)
    for j in range(n // LANE):
        part = val[:, j * LANE:(j + 1) * LANE]
        acc = acc + part * part
    acc = jnp.concatenate([acc] * (LANE // h), axis=0)
    return jnp.sum(acc.T, axis=0, keepdims=True)


def kernel(
    nr, nc, inv, tiles, sino, sol, res,
    fa, ba, y0, yb, bacc, fpart, drecv, xb, vfull, ray, vox, relay, vrow, sdir,
    bsend, brecv, vgat, fsend, frecv, zbuf, cbuf,
    bs, br, vs, vr, ds_, dr, fs, fr, gs, gr, hs, hr, zs, zr, cs, cr,
):
    mr = lax.axis_index("row")
    mc = lax.axis_index("col")
    nch = nc // 2
    chip = mc // 2
    core = mc % 2
    partner = chip * 2 + (1 - core)
    tile = tiles.shape[1]
    mb, z = sino.shape
    nb = sol.shape[0]
    tr, tc = mb // tile, nb // tile
    sv, sr = nb // nr, mb // nc
    hz = z // 2

    inner = (mr == 1) | (mr == 2)
    outer = jnp.logical_not(inner)
    left = mr < 2
    mate = mr + 1 - 2 * lax.rem(mr, 2)
    cross = jnp.where(left, 2, 1)
    far = jnp.where(left, 3, 0)
    early = jnp.where(inner, far, mate)
    late = jnp.where(inner, mate, far)

    barrier = pltpu.get_barrier_semaphore()
    for s in range(1, nr):
        pl.semaphore_signal(barrier, 1, device_id=(lax.rem(mr + s, nr), mc), device_id_type=MESH)
    for s in range(1, nc):
        pl.semaphore_signal(barrier, 1, device_id=(mr, lax.rem(mc + s, nc)), device_id_type=MESH)

    sent = []

    def copy_to(src, dst, ssem, rsem, row, col):
        return pltpu.make_async_remote_copy(
            src_ref=src, dst_ref=dst, send_sem=ssem, recv_sem=rsem,
            device_id=(row, col), device_id_type=MESH)

    def send(src, dst, ssem, rsem, row, col):
        copy = copy_to(src, dst, ssem, rsem, row, col)
        copy.start()
        sent.append(copy)
        return copy

    def block(first, size):
        return pl.ds(pl.multiple_of(first, size), size)

    def pick(i, j):
        slot = inv[i * tc + j]
        values = tiles[jnp.maximum(slot, 0)]
        return jnp.where(slot >= 0, values, jnp.zeros_like(values))

    def column(row, h):
        return jnp.broadcast_to(row, (z, z)).T[h * hz:(h + 1) * hz]

    def wide(col, n):
        return jnp.concatenate([col] * (n // LANE), axis=1)

    def merge(a, b):
        lane = lax.broadcasted_iota(jnp.int32, (1, z), 1)
        return jnp.where(lane < hz, a, b)

    def share(vec, buf, n, me, ssem, rsem, over_row):
        buf[me] = jnp.broadcast_to(vec, (8, z))
        copies = []
        for s in range(1, n):
            peer = lax.rem(me + s, n)
            place = (peer, mc) if over_row else (mr, peer)
            copies.append(send(buf.at[me], buf.at[me], ssem.at[s], rsem.at[s], *place))

        def finish():
            for copy in copies:
                copy.wait_recv()
            total = buf[0]
            for q in range(1, n):
                total = total + buf[q]
            return total[:1]

        return finish

    def share_z(vec, n, h):
        return share(vec, zbuf.at[n, h], nr, mr, zs.at[n, h], zr.at[n, h], True)

    def share_c(vec, n, h):
        return share(vec, cbuf.at[n, h], nc, mc, cs.at[n, h], cr.at[n, h], False)

    def back_part(k, h, dest):
        cols = block(dest * sv, sv)
        if k == 0:
            if h == 0:
                val = dot(y0[...], fa[:, cols])
                bacc[1, dest] = val[hz:]
                return val[:hz]
            return bacc[1, dest]
        val = bacc[h, dest]
        q = lax.rem(chip + 1, nch) * 2
        for i in range(2):
            val = val + dot(yb[k, h, q + i], fa[block((q + i) * sr, sr), cols])
        return val

    def back_grow(k, h, q, fresh):
        for d in range(nr):
            cols = slice(d * sv, (d + 1) * sv)
            val = dot(yb[k, h, q], fa[block(q * sr, sr), cols])
            val = val + dot(yb[k, h, q + 1], fa[block((q + 1) * sr, sr), cols])
            bacc[h, d] = val if fresh else bacc[h, d] + val

    def back_start(k, h):
        col_pack(bsend.at[k, h, 0], back_part(k, h, jnp.where(inner, cross, far)))
        slot = jnp.where(inner, 3, 0)
        send(bsend.at[k, h, 0], brecv.at[k, h, slot], bs.at[k, h, 0], br.at[k, h, slot],
             jnp.where(inner, cross, mate), mc)
        relay[h] = back_part(k, h, jnp.where(inner, far, cross))

        @pl.when(outer)
        def _():
            col_pack(bsend.at[k, h, 1], relay[h])
            copy_to(bsend.at[k, h, 1], brecv.at[k, h, 1], bs.at[k, h, 1], br.at[k, h, 1], cross, mc).start()

        col_pack(bsend.at[k, h, 2], back_part(k, h, mate))
        send(bsend.at[k, h, 2], brecv.at[k, h, 2], bs.at[k, h, 2], br.at[k, h, 2], mate, mc)
        vox[k, h] = back_part(k, h, mr)

    def back_arrived(k, h, slot):
        copy_to(bsend.at[k, h, slot], brecv.at[k, h, slot], bs.at[k, h, slot], br.at[k, h, slot],
                mate, mc).wait_recv()
        return col_unpack(brecv.at[k, h, slot], hz)

    def back_relay(k, h):
        @pl.when(inner)
        def _():
            col_pack(bsend.at[k, h, 1], relay[h] + back_arrived(k, h, 0))
            copy_to(bsend.at[k, h, 1], brecv.at[k, h, 1], bs.at[k, h, 1], br.at[k, h, 1], far, mc).start()

        sent.append(copy_to(bsend.at[k, h, 1], brecv.at[k, h, 1], bs.at[k, h, 1], br.at[k, h, 1], mate, mc))

    def back_sum(k, h):
        @pl.when(inner)
        def _():
            vox[k, h] = vox[k, h] + back_arrived(k, h, 3)

        total = vox[k, h] + back_arrived(k, h, 2)
        return total + back_arrived(k, h, 1)

    def fwd_grow(k, h, origin, fresh):
        for q in range(nch):
            cols = slice(2 * q * sr, 2 * (q + 1) * sr)
            val = dot(xb[h, origin], ba[block(origin * sv, sv), cols])
            for i in range(2):
                half = val[:, i * sr:(i + 1) * sr]
                fpart[k, h, 2 * q + i] = half if fresh else fpart[k, h, 2 * q + i] + half

    def vox_take(k, h, origin):
        val = col_unpack(vgat.at[k, h, origin], hz)
        vfull[h, origin] = val
        xb[h, origin] = val.astype(jnp.bfloat16)

    def passed(k, h, origin, n, row):
        own = vgat.at[k, h, origin]
        return copy_to(own, own, vs.at[k, h, n], vr.at[k, h, origin], row, mc)

    def vox_send(k, h):
        @pl.when(inner)
        def _():
            passed(k, h, mr, 2, far).start()

        own = vgat.at[k, h, mr]
        send(own, own, vs.at[k, h, 1], vr.at[k, h, mr], cross, mc)
        send(own, own, vs.at[k, h, 0], vr.at[k, h, mr], mate, mc)

    def vox_early(k, h):
        @pl.when(inner)
        def _():
            passed(k, h, far, 3, mate).wait_recv()
            passed(k, h, far, 3, mate).start()

        @pl.when(outer)
        def _():
            passed(k, h, mate, 0, mate).wait_recv()

        vox_take(k, h, early)

    def fwd_send(k, h):
        local = []
        for s in list(range(1, nch)) + [0]:
            q = lax.rem(chip + s, nch) * 2
            val = dot(xb[h, late], ba[block(late * sv, sv), block(q * sr, 2 * sr)])
            for i in range(2):
                fpart[k, h, q + i] = fpart[k, h, q + i] + val[:, i * sr:(i + 1) * sr]
            local.append(send(fpart.at[k, h, q + 1 - core], drecv.at[k, h, s],
                              ds_.at[k, h, s], dr.at[k, h, s], mr, partner))
        return local

    def fwd_pass(k, h, local):
        copies = []
        for s, other in zip(list(range(1, nch)) + [0], local):
            q = lax.rem(chip + s, nch) * 2 + core
            other.wait_recv()
            part = fpart[k, h, q] + drecv[k, h, s]
            if s:
                col_pack(fsend.at[k, h, s], part)
                copies.append(send(fsend.at[k, h, s], frecv.at[k, h, s], fs.at[k, h, s], fr.at[k, h, s], mr, q))
            else:
                ray[k + 1, h] = part
        return copies

    def fwd_sum(k, h, copies):
        total = ray[k + 1, h]
        for i, copy in enumerate(copies):
            copy.wait_recv()
            total = total + col_unpack(frecv.at[k, h, i + 1], hz)
        return total

    def flip(first, last):
        @pl.loop(first, last)
        def _(d):
            for j in range(sv // LANE):
                cols = slice(j * LANE, (j + 1) * LANE)
                both = jnp.concatenate([vfull[0, d, :, cols], vfull[1, d, :, cols]], axis=0)
                vrow[block(d * sv + j * LANE, LANE), :] = both.T

    alphas = [[None, None] for _ in range(ITERS)]
    betas = [[None, None] for _ in range(ITERS + 1)]
    run = {}

    def update_dir(k):
        alpha = merge(*alphas[k])
        inv_alpha = 1.0 / alpha
        if k == 0:
            run["rho_bar"] = alpha
            sdir[...] = vrow[...] * inv_alpha
        else:
            theta = run["sine"] * alpha
            run["rho_bar"] = -run["cosine"] * alpha
            sdir[...] = vrow[...] * inv_alpha - (theta / run["rho"]) * sdir[...]

    def update_sol(k):
        beta = merge(*betas[k + 1])
        rho_bar = run["rho_bar"]
        rho = jnp.sqrt(rho_bar * rho_bar + beta * beta)
        run["rho"] = rho
        run["cosine"] = rho_bar / rho
        run["sine"] = beta / rho
        phi = run["cosine"] * run["phi_bar"]
        run["phi_bar"] = run["sine"] * run["phi_bar"]
        step = (phi / rho) * sdir[...]
        sol[...] = step if k == 0 else sol[...] + step

    def half(h):
        beta_of = None
        for k in range(ITERS):
            back_start(k, h)
            yield
            back_relay(k, h)
            yield
            total = back_sum(k, h)
            if k:
                betas[k][h] = root(beta_of)
            beta = betas[k][h]
            raw = total * wide(column(1.0 / beta, h), sv)
            if k:
                raw = raw - wide(column(beta / alphas[k - 1][h], h), sv) * vox[k - 1, h]
            vox[k, h] = raw
            col_pack(vgat.at[k, h, mr], raw)
            vox_send(k, h)
            alpha_of = share_z(row_squares(raw), 2 * k + 1, h)
            vox_take(k, h, mr)
            if k == 0 and h == 0:
                build_ba()
            fwd_grow(k, h, mr, True)
            if k and h:
                update_sol(k - 1)
            yield
            vox_early(k, h)
            fwd_grow(k, h, early, False)
            yield
            passed(k, h, cross, 0, mate).wait_recv()
            vox_take(k, h, cross)
            fwd_grow(k, h, cross, False)
            yield
            passed(k, h, late, 0, mate).wait_recv()
            vox_take(k, h, late)
            local = fwd_send(k, h)
            alpha_of = share_c(alpha_of(), 2 * k + 1, h)
            yield
            copies = fwd_pass(k, h, local)
            if h:
                flip(0, nr)
            yield
            total = fwd_sum(k, h, copies)
            alpha = root(alpha_of)
            alphas[k][h] = alpha
            raw = total * wide(column(1.0 / alpha, h), sr)
            raw = raw - wide(column(alpha / beta, h), sr) * ray[k, h]
            n = 2 * k + 2
            if k + 1 == ITERS:
                beta_of = share_c(row_squares(raw), n, h)
                if h:
                    update_dir(k)
                yield
                beta_of = share_z(beta_of(), n, h)
                yield
                betas[k + 1][h] = root(beta_of)
                return
            ray[k + 1, h] = raw
            own = yb.at[k + 1, h, mc]
            own[...] = raw.astype(jnp.bfloat16)
            across = [send(own, own, gs.at[k, h, 0], gr.at[k, h, 0], mr, partner)]
            for s in range(1, nch):
                peer = lax.rem(chip + s, nch) * 2 + core
                across.append(send(own, own, gs.at[k, h, s], gr.at[k, h, s], mr, peer))
            beta_of = share_c(row_squares(raw), n, h)
            if h:
                update_dir(k)
            yield
            across[0].wait_recv()
            back_grow(k + 1, h, chip * 2, True)
            yield
            hand = [None]
            for s in range(1, nch):
                across[s].wait_recv()
                origin = lax.rem(chip + nch - s, nch) * 2 + core
                given = yb.at[k + 1, h, origin]
                hand.append(send(given, given, hs.at[k, h, s], hr.at[k, h, s], mr, partner))
            beta_of = share_z(beta_of(), n, h)
            yield
            for s in range(1, nch):
                hand[s].wait_recv()
                if s + 1 < nch:
                    back_grow(k + 1, h, lax.rem(chip + nch - s, nch) * 2, False)

    def build_ba():
        @pl.loop(0, tc)
        def _(j):
            for i in range(tr):
                ba[block(j * tile, tile), i * tile:(i + 1) * tile] = pick(i, j).T

    @pl.loop(0, tr)
    def _(i):
        for j in range(tc):
            fa[block(i * tile, tile), j * tile:(j + 1) * tile] = pick(i, j)

    total = squares(sino[...])
    pl.semaphore_wait(barrier, nr - 1 + nc - 1)
    beta_of = share_z(total, 0, 0)
    for i in range(tr):
        y0[:, i * tile:(i + 1) * tile] = sino[i * tile:(i + 1) * tile, :].T.astype(jnp.bfloat16)
    own = sino[block(mc * sr, sr), :].T
    ray[0, 0] = own[:hz]
    ray[0, 1] = own[hz:]
    beta = root(beta_of)
    betas[0] = [beta, beta]
    run["phi_bar"] = beta
    live = [half(0), half(1)]
    while live:
        for one in list(live):
            try:
                next(one)
            except StopIteration:
                live.remove(one)
    update_sol(ITERS - 1)
    res[...] = jnp.broadcast_to(run["phi_bar"], res.shape)
    for copy in sent:
        copy.wait_send()

    @pl.when(inner)
    def _():
        for k in range(ITERS):
            for h in range(2):
                passed(k, h, mr, 2, far).wait_send()
                passed(k, h, far, 3, mate).wait_send()


def body(nr, nc, tile_values, tile_rows, tile_cols, tile_count, sinogram):
    values = tile_values[0, 0]
    slots, tile = values.shape[0], values.shape[1]
    mb, z = sinogram.shape
    nb = TC * tile
    tr = mb // tile
    sv, sr = nb // nr, mb // nc
    if nr != 4 or nc % 2 or sr % LANE or sv % LANE or z != LANE:
        return body_rows(nr, nc, tile_values, tile_rows, tile_cols, tile_count, sinogram)
    place = tile_rows[0, 0] * TC + tile_cols[0, 0]
    ids = jnp.arange(slots, dtype=jnp.int32)
    place = jnp.where(ids < tile_count[0, 0], place, -1)
    hit = place[None, :] == jnp.arange(tr * TC, dtype=jnp.int32)[:, None]
    inv = jnp.sum(jnp.where(hit, ids[None, :] + 1, 0), axis=1, dtype=jnp.int32) - 1
    nch, hz = nc // 2, z // 2
    f32, bf16, i16 = jnp.float32, jnp.bfloat16, jnp.int16
    dma, vmem_of = pltpu.SemaphoreType.DMA, pltpu.VMEM
    vmem = pl.BlockSpec(memory_space=pltpu.VMEM)
    pb, pf = sv // LANE * hz + PAD, sr // LANE * hz + PAD
    norms = 2 * ITERS + 1
    scratch = [
        vmem_of((mb, nb), bf16), vmem_of((nb, mb), bf16), vmem_of((z, mb), bf16),
        vmem_of((ITERS, 2, nc, hz, sr), bf16), vmem_of((2, nr, hz, sv), f32),
        vmem_of((ITERS, 2, nc, hz, sr), f32), vmem_of((ITERS, 2, nch, hz, sr), f32),
        vmem_of((2, nr, hz, sv), bf16), vmem_of((2, nr, hz, sv), f32),
        vmem_of((ITERS + 1, 2, hz, sr), f32), vmem_of((ITERS, 2, hz, sv), f32), vmem_of((2, hz, sv), f32),
        vmem_of((nb, z), f32), vmem_of((nb, z), f32),
        vmem_of((ITERS, 2, nr, pb, LANE), i16), vmem_of((ITERS, 2, nr, pb, LANE), i16),
        vmem_of((ITERS, 2, nr, pb, LANE), i16),
        vmem_of((ITERS, 2, nch, pf, LANE), i16), vmem_of((ITERS, 2, nch, pf, LANE), i16),
        vmem_of((norms, 2, nr, 8, z), f32), vmem_of((norms, 2, nc, 8, z), f32),
    ] + [dma((ITERS, 2, nr))] * 4 + [dma((ITERS, 2, nch))] * 8 + [
        dma((norms, 2, nr)), dma((norms, 2, nr)), dma((norms, 2, nc)), dma((norms, 2, nc)),
    ]
    sol, res = pl.pallas_call(
        functools.partial(kernel, nr, nc),
        out_shape=(jax.ShapeDtypeStruct((nb, z), f32), jax.ShapeDtypeStruct((8, z), f32)),
        in_specs=[pl.BlockSpec(memory_space=pltpu.SMEM), vmem, vmem],
        out_specs=(vmem, vmem),
        scratch_shapes=scratch,
        compiler_params=pltpu.CompilerParams(
            collective_id=0, has_side_effects=True, vmem_limit_bytes=60 * 1024 * 1024),
    )(inv, values, sinogram)
    return sol, res[0]


def solution(mesh):
    nr, nc = mesh.shape["row"], mesh.shape["col"]
    in_specs = (
        P("row", "col", None, None, None),
        P("row", "col", None),
        P("row", "col", None),
        P("row", "col"),
        P("row", None),
    )
    return jax.shard_map(
        functools.partial(body, nr, nc), mesh=mesh, in_specs=in_specs,
        out_specs=(P("col", None), P()), check_vma=False)
```

```python
import functools

import jax
import jax.numpy as jnp
from jax import lax
from jax.experimental import pallas as pl
from jax.experimental.pallas import tpu as pltpu
from jax.sharding import PartitionSpec as P

TC = 16
ITERS = 3
EPSILON = 1e-06
PAD = 16
TOP = 32000.0
FINE = 64.0
LANE = 128
GRANT = 53000 * 1024
ORDER = [0, 1] * 10 * ITERS
MESH = pl.DeviceIdType.MESH


def pack(val):
    top = jnp.max(jnp.abs(val), axis=0, keepdims=True)
    exponent = jnp.ceil(jnp.log2(jnp.maximum(top, 1e-30)))
    scale = TOP * jnp.exp2(-exponent)
    coded = jnp.round(jnp.clip(val * scale, -32767.0, 32767.0))
    coded = coded.astype(jnp.int32).astype(jnp.int16)
    rows = jnp.broadcast_to(exponent, (PAD, val.shape[1]))
    return coded, rows.astype(jnp.int32).astype(jnp.int16)


def store_packet(ref, val):
    n = val.shape[0]
    coded, rows = pack(val)
    ref[pl.ds(0, n), :] = coded
    ref[pl.ds(n, PAD), :] = rows


def load_packet(ref):
    n = ref.shape[0] - PAD
    exponent = ref[pl.ds(n, PAD), :].astype(jnp.int32).astype(jnp.float32)[:1]
    scale = jnp.exp2(exponent) * (1.0 / TOP)
    return ref[pl.ds(0, n), :].astype(jnp.int32).astype(jnp.float32) * scale


def dot(a, b):
    return jnp.dot(a, b, preferred_element_type=jnp.float32)


def root(total_of):
    return jnp.sqrt(total_of() + EPSILON)


def squares(vec):
    return jnp.sum(vec * vec, axis=0, keepdims=True)


def kernel_rows(
    nr, nc, inv, tiles, sino, sol, res,
    facc, bacc, sq, fa, ba, ybf, xbf, ray, vox, vfull, sdir,
    bsend, brecv, vgat, dsend, drecv, fsend, frecv, rgat, nrow, ncol, nlast,
    bs, br, vs, vr, ds_, dr, fs, fr, gs, gr, hs, hr, rs, rr, cs, cr, ls, lr,
):
    mr = lax.axis_index("row")
    mc = lax.axis_index("col")
    nch = nc // 2
    chip = mc // 2
    core = mc % 2
    partner = chip * 2 + (1 - core)
    tile = tiles.shape[1]
    mb, z = sino.shape
    nb = sol.shape[0]
    tr, tc = mb // tile, nb // tile
    sv, sr = nb // nr, mb // nc

    barrier = pltpu.get_barrier_semaphore()
    for s in range(1, nr):
        pl.semaphore_signal(barrier, 1, device_id=(lax.rem(mr + s, nr), mc), device_id_type=MESH)
    for s in range(1, nc):
        pl.semaphore_signal(barrier, 1, device_id=(mr, lax.rem(mc + s, nc)), device_id_type=MESH)

    def send(src, dst, ssem, rsem, row, col):
        copy = pltpu.make_async_remote_copy(
            src_ref=src, dst_ref=dst, send_sem=ssem, recv_sem=rsem,
            device_id=(row, col), device_id_type=MESH)
        copy.start()
        sent.append(copy)
        return copy

    sent = []

    def pick(i, j):
        slot = inv[i * tc + j]
        block = tiles[jnp.maximum(slot, 0)]
        return jnp.where(slot >= 0, block, jnp.zeros_like(block))

    @pl.loop(0, tc)
    def _(j):
        first = pl.multiple_of(j * tile, tile)
        for i in range(tr):
            ba[pl.ds(first, tile), i * tile:(i + 1) * tile] = pick(i, j).T

    def share(vec, buf, n, me, ssem, rsem, over_row):
        buf[me] = jnp.broadcast_to(vec, (8, z))
        copies = []
        for s in range(1, n):
            peer = lax.rem(me + s, n)
            place = (peer, mc) if over_row else (mr, peer)
            copies.append(send(buf.at[me], buf.at[me], ssem.at[s], rsem.at[s], *place))

        def finish():
            for copy in copies:
                copy.wait_recv()
            total = buf[0]
            for q in range(1, n):
                total = total + buf[q]
            return total[:1]

        return finish

    line = nr == 4
    inner = (mr == 1) | (mr == 2)
    left = mr < 2
    mate = mr + 1 - 2 * lax.rem(mr, 2)
    cross = jnp.where(left, 2, 1)
    far = jnp.where(left, 3, 0)
    early = jnp.where(inner, far, mate)
    late = jnp.where(inner, mate, far)
    inner_sent = []

    def row_copy(src, dst, ssem, rsem, row):
        return pltpu.make_async_remote_copy(
            src_ref=src, dst_ref=dst, send_sem=ssem, recv_sem=rsem,
            device_id=(row, mc), device_id_type=MESH)

    def back_part(k, dest):
        rows = pl.ds(pl.multiple_of(dest * sv, sv), sv)
        if k == 0:
            return dot(ba[rows, :], ybf[...])
        late = lax.rem(chip + 1, nch) * 2 * sr
        cols = pl.ds(pl.multiple_of(late, 2 * sr), 2 * sr)
        return bacc[rows, :] + dot(ba[rows, cols], ybf[cols, :])

    def back_arrived(k, slot):
        row_copy(bsend.at[k, slot], brecv.at[k, slot], bs.at[k, slot], br.at[k, slot], mate).wait_recv()

    def back_start(k):
        if line:
            store_packet(bsend.at[k, 0], back_part(k, jnp.where(inner, cross, far)))
            slot = jnp.where(inner, 3, 0)
            send(bsend.at[k, 0], brecv.at[k, slot], bs.at[k, 0], br.at[k, slot],
                 jnp.where(inner, cross, mate), mc)
            part = back_part(k, jnp.where(inner, far, cross))

            @pl.when(jnp.logical_not(inner))
            def _():
                store_packet(bsend.at[k, 1], part)

            @pl.when(inner)
            def _():
                back_arrived(k, 0)
                store_packet(bsend.at[k, 1], part + load_packet(brecv.at[k, 0]))

            send(bsend.at[k, 1], brecv.at[k, 1], bs.at[k, 1], br.at[k, 1], jnp.where(inner, far, cross), mc)
            store_packet(bsend.at[k, 2], back_part(k, mate))
            send(bsend.at[k, 2], brecv.at[k, 2], bs.at[k, 2], br.at[k, 2], mate, mc)
            vox[k] = back_part(k, mr)
            return None
        copies = []
        for s in list(range(1, nr)) + [0]:
            dest = lax.rem(mr + s, nr)
            part = back_part(k, dest)
            if s:
                store_packet(bsend.at[k, s], part)
                copies.append(send(bsend.at[k, s], brecv.at[k, s], bs.at[k, s], br.at[k, s], dest, mc))
            else:
                vox[k] = part
        return copies

    def back_sum(k, copies):
        if line:
            @pl.when(inner)
            def _():
                back_arrived(k, 3)
                vox[k] = vox[k] + load_packet(brecv.at[k, 3])

            total = vox[k]
            for slot in (2, 1):
                back_arrived(k, slot)
                total = total + load_packet(brecv.at[k, slot])
            return total
        total = vox[k]
        for i, copy in enumerate(copies):
            copy.wait_recv()
            total = total + load_packet(brecv.at[k, i + 1])
        return total

    def vox_take(k, origin):
        val = load_packet(vgat.at[k, origin])
        rows = pl.ds(pl.multiple_of(origin * sv, sv), sv)
        vfull[rows, :] = val
        xbf[rows, :] = val.astype(jnp.bfloat16)

    def grow(acc, mat, vec, first, depth, fresh):
        cols = pl.ds(pl.multiple_of(first, depth), depth)

        @pl.loop(0, acc.shape[0] // sv)
        def _(i):
            rows = pl.ds(pl.multiple_of(i * sv, sv), sv)
            val = dot(mat[rows, cols], vec[cols, :])
            acc[rows, :] = val if fresh else acc[rows, :] + val

    def vox_gather(k):
        store_packet(vgat.at[k, mr], vox[k])
        if line:
            def passed(origin, n, row):
                return row_copy(vgat.at[k, origin], vgat.at[k, origin], vs.at[k, n], vr.at[k, origin], row)

            @pl.when(inner)
            def _():
                passed(mr, 2, far).start()

            send(vgat.at[k, mr], vgat.at[k, mr], vs.at[k, 1], vr.at[k, mr], cross, mc)
            send(vgat.at[k, mr], vgat.at[k, mr], vs.at[k, 0], vr.at[k, mr], mate, mc)
            inner_sent.append(passed(mr, 2, far))
            inner_sent.append(passed(far, 3, mate))
            vox_take(k, mr)
            grow(facc, fa, xbf, mr * sv, sv, True)

            @pl.when(inner)
            def _():
                passed(far, 3, mate).wait_recv()
                passed(far, 3, mate).start()

            @pl.when(jnp.logical_not(inner))
            def _():
                passed(mate, 0, mate).wait_recv()

            vox_take(k, early)
            grow(facc, fa, xbf, early * sv, sv, False)
            passed(cross, 0, mate).wait_recv()
            vox_take(k, cross)
            grow(facc, fa, xbf, cross * sv, sv, False)
            passed(late, 0, mate).wait_recv()
            vox_take(k, late)
        else:
            copies = [
                send(vgat.at[k, mr], vgat.at[k, mr], vs.at[k, s], vr.at[k, s], lax.rem(mr + s, nr), mc)
                for s in range(1, nr)
            ]
            for copy in copies:
                copy.wait_recv()
            for q in range(nr):
                vox_take(k, q)
        return share(squares(vfull[...]), ncol.at[k], nc, mc, cs.at[k], cr.at[k], False)

    def fwd_part(first):
        rows = pl.ds(first, sr)
        if line:
            cols = pl.ds(pl.multiple_of(late * sv, sv), sv)
            return facc[rows, :] + dot(fa[rows, cols], xbf[cols, :])
        return dot(fa[rows, :], xbf[...])

    def fwd_start(k):
        order = list(range(1, nch)) + [0]
        local = []
        for s in order:
            q = lax.rem(chip + s, nch)
            first = pl.multiple_of((q * 2 + 1 - core) * sr, sr)
            dsend[k, s] = fwd_part(first)
            local.append(send(dsend.at[k, s], drecv.at[k, s], ds_.at[k, s], dr.at[k, s], mr, partner))
        copies = []
        for s, other in zip(order, local):
            q = lax.rem(chip + s, nch)
            first = pl.multiple_of((q * 2 + core) * sr, sr)
            part = fwd_part(first)
            other.wait_recv()
            part = part + drecv[k, s]
            if s:
                store_packet(fsend.at[k, s], part)
                copies.append(send(fsend.at[k, s], frecv.at[k, s], fs.at[k, s], fr.at[k, s], mr, q * 2 + core))
            else:
                ray[k + 1] = part
        return copies

    def fwd_sum(k, copies):
        total = ray[k + 1]
        for i, copy in enumerate(copies):
            copy.wait_recv()
            total = total + load_packet(frecv.at[k, i + 1])
        return total

    def ray_gather(k):
        store_packet(rgat.at[k, mc], ray[k + 1])
        across = [send(rgat.at[k, mc], rgat.at[k, mc], gs.at[k, 0], gr.at[k, 0], mr, partner)]
        for s in range(1, nch):
            peer = lax.rem(chip + s, nch) * 2 + core
            across.append(send(rgat.at[k, mc], rgat.at[k, mc], gs.at[k, s], gr.at[k, s], mr, peer))
        hand = [None]

        def take(origin):
            val = load_packet(rgat.at[k, origin])
            sq[origin] = jnp.broadcast_to(squares(val), (8, z))
            ybf[pl.ds(pl.multiple_of(origin * sr, sr), sr), :] = val.astype(jnp.bfloat16)

        take(mc)
        across[0].wait_recv()
        take(partner)
        grow(bacc, ba, ybf, chip * 2 * sr, 2 * sr, True)
        for s in range(1, nch):
            across[s].wait_recv()
            origin = lax.rem(chip + nch - s, nch) * 2 + core
            hand.append(send(rgat.at[k, origin], rgat.at[k, origin], hs.at[k, s], hr.at[k, s], mr, partner))
            take(origin)
        for s in range(1, nch):
            hand[s].wait_recv()
            origin = lax.rem(chip + nch - s, nch) * 2
            take(origin + 1 - core)
            if s + 1 < nch:
                grow(bacc, ba, ybf, origin * sr, 2 * sr, False)
        total = jnp.zeros((1, z), jnp.float32)
        for q in range(nc):
            total = total + sq[q][:1]
        return share(total, nrow.at[k + 1], nr, mr, rs.at[k + 1], rr.at[k + 1], True)

    ybf[...] = sino[...].astype(jnp.bfloat16)
    total = squares(sino[...])
    pl.semaphore_wait(barrier, nr - 1 + nc - 1)
    beta_of = share(total, nrow.at[0], nr, mr, rs.at[0], rr.at[0], True)
    copies = back_start(0)

    @pl.loop(0, tr)
    def _(i):
        first = pl.multiple_of(i * tile, tile)
        for j in range(tc):
            fa[pl.ds(first, tile), j * tile:(j + 1) * tile] = pick(i, j)

    beta = root(beta_of)
    ray[0] = sino[pl.ds(pl.multiple_of(mc * sr, sr), sr), :] * (1.0 / beta)
    vox[0] = back_sum(0, copies) * (1.0 / beta)
    alpha_of = vox_gather(0)
    phi_bar = beta
    for k in range(ITERS):
        copies = fwd_start(k)
        alpha = root(alpha_of)
        inv_alpha = 1.0 / alpha
        if k == 0:
            rho_bar = alpha
            sdir[...] = vfull[...] * inv_alpha
        else:
            theta = sine * alpha
            rho_bar = -cosine * alpha
            sdir[...] = vfull[...] * inv_alpha - (theta / rho) * sdir[...]
        vox[k] = vox[k] * inv_alpha
        ray_raw = fwd_sum(k, copies) * inv_alpha - alpha * ray[k]
        last = k + 1 == ITERS
        if last:
            total = share(squares(ray_raw), nlast, nc, mc, ls, lr, False)()
            beta = root(share(total, nrow.at[k + 1], nr, mr, rs.at[k + 1], rr.at[k + 1], True))
        else:
            ray[k + 1] = ray_raw
            beta_of = ray_gather(k)
            copies = back_start(k + 1)
            beta = root(beta_of)
            ray[k + 1] = ray[k + 1] * (1.0 / beta)
        rho = jnp.sqrt(rho_bar * rho_bar + beta * beta)
        cosine = rho_bar / rho
        sine = beta / rho
        phi = cosine * phi_bar
        phi_bar = sine * phi_bar
        step = (phi / rho) * sdir[...]
        sol[...] = step if k == 0 else sol[...] + step
        if not last:
            vox[k + 1] = back_sum(k + 1, copies) * (1.0 / beta) - beta * vox[k]
            alpha_of = vox_gather(k + 1)
    res[...] = jnp.broadcast_to(phi_bar, res.shape)
    for copy in sent:
        copy.wait_send()
    if line:
        @pl.when(inner)
        def _():
            for copy in inner_sent:
                copy.wait_send()


def body_rows(nr, nc, tile_values, tile_rows, tile_cols, tile_count, sinogram):
    values = tile_values[0, 0]
    slots, tile = values.shape[0], values.shape[1]
    mb, z = sinogram.shape
    nb = TC * tile
    tr = mb // tile
    place = tile_rows[0, 0] * TC + tile_cols[0, 0]
    ids = jnp.arange(slots, dtype=jnp.int32)
    place = jnp.where(ids < tile_count[0, 0], place, -1)
    hit = place[None, :] == jnp.arange(tr * TC, dtype=jnp.int32)[:, None]
    inv = jnp.sum(jnp.where(hit, ids[None, :] + 1, 0), axis=1, dtype=jnp.int32) - 1
    nch = nc // 2
    sv, sr = nb // nr, mb // nc
    f32, bf16, i16 = jnp.float32, jnp.bfloat16, jnp.int16
    dma = pltpu.SemaphoreType.DMA
    vmem = pl.BlockSpec(memory_space=pltpu.VMEM)
    scratch = [
        pltpu.VMEM((mb, z), f32), pltpu.VMEM((nb, z), f32), pltpu.VMEM((nc, 8, z), f32),
        pltpu.VMEM((mb, nb), bf16), pltpu.VMEM((nb, mb), bf16),
        pltpu.VMEM((mb, z), bf16), pltpu.VMEM((nb, z), bf16),
        pltpu.VMEM((ITERS + 1, sr, z), f32), pltpu.VMEM((ITERS, sv, z), f32),
        pltpu.VMEM((nb, z), f32), pltpu.VMEM((nb, z), f32),
        pltpu.VMEM((ITERS, nr, sv + PAD, z), i16), pltpu.VMEM((ITERS, nr, sv + PAD, z), i16),
        pltpu.VMEM((ITERS, nr, sv + PAD, z), i16),
        pltpu.VMEM((ITERS, nch, sr, z), f32), pltpu.VMEM((ITERS, nch, sr, z), f32),
        pltpu.VMEM((ITERS, nch, sr + PAD, z), i16), pltpu.VMEM((ITERS, nch, sr + PAD, z), i16),
        pltpu.VMEM((ITERS, nc, sr + PAD, z), i16),
        pltpu.VMEM((ITERS + 1, nr, 8, z), f32), pltpu.VMEM((ITERS, nc, 8, z), f32),
        pltpu.VMEM((nc, 8, z), f32),
        dma((ITERS, nr)), dma((ITERS, nr)), dma((ITERS, nr)), dma((ITERS, nr)),
        dma((ITERS, nch)), dma((ITERS, nch)), dma((ITERS, nch)), dma((ITERS, nch)),
        dma((ITERS, nch)), dma((ITERS, nch)), dma((ITERS, nch)), dma((ITERS, nch)),
        dma((ITERS + 1, nr)), dma((ITERS + 1, nr)), dma((ITERS, nc)), dma((ITERS, nc)),
        dma((nc,)), dma((nc,)),
    ]
    sol, res = pl.pallas_call(
        functools.partial(kernel_rows, nr, nc),
        out_shape=(jax.ShapeDtypeStruct((nb, z), f32), jax.ShapeDtypeStruct((8, z), f32)),
        in_specs=[pl.BlockSpec(memory_space=pltpu.SMEM), vmem, vmem],
        out_specs=(vmem, vmem),
        scratch_shapes=scratch,
        compiler_params=pltpu.CompilerParams(
            collective_id=0, has_side_effects=True, vmem_limit_bytes=60 * 1024 * 1024),
    )(inv, values, sinogram)
    return sol, res[0]


def col_pack(ref, val):
    h, n = val.shape
    groups = h // PAD
    mag = jnp.abs(val)
    top = mag[:PAD]
    for g in range(1, groups):
        top = jnp.maximum(top, mag[g * PAD:(g + 1) * PAD])
    top = jnp.max(top, axis=1, keepdims=True)
    exponent = jnp.ceil(jnp.log2(jnp.maximum(top, 1e-30)) * FINE)
    scale = jnp.concatenate([TOP * jnp.exp2(exponent * (-1.0 / FINE))] * groups, axis=0)
    coded = jnp.round(val * scale).astype(jnp.int32).astype(jnp.int16)
    for j in range(n // LANE):
        ref[pl.ds(j * h, h), :] = coded[:, j * LANE:(j + 1) * LANE]
    ref[pl.ds(n // LANE * h, PAD), :] = jnp.broadcast_to(exponent, (PAD, LANE)).astype(jnp.int32).astype(jnp.int16)


def col_unpack(ref, h):
    blocks = (ref.shape[0] - PAD) // h
    exponent = ref[pl.ds(blocks * h, PAD), :].astype(jnp.int32).astype(jnp.float32)
    scale = jnp.concatenate([jnp.exp2(exponent * (1.0 / FINE)) * (1.0 / TOP)] * (h // PAD), axis=0)
    return jnp.concatenate(
        [ref[pl.ds(j * h, h), :].astype(jnp.int32).astype(jnp.float32) * scale for j in range(blocks)], axis=1)


def row_squares(val):
    h, n = val.shape
    acc = jnp.zeros((h, LANE), jnp.float32)
    for j in range(n // LANE):
        part = val[:, j * LANE:(j + 1) * LANE]
        acc = acc + part * part
    acc = jnp.concatenate([acc] * (LANE // h), axis=0)
    return jnp.sum(acc.T, axis=0, keepdims=True)


def kernel(
    nr, nc, place_of, tiles_in, sino_in, sol, sdir, res,
    tiles, sino, inv_row, inv,
    fa, ba, y0, yb, bacc, fpart, drecv, xb, vfull, ray, vox, relay, vrow,
    bsend, brecv, vgat, fsend, frecv, zbuf, cbuf,
    bs, br, vs, vr, ds_, dr, fs, fr, gs, gr, hs, hr, zs, zr, cs, cr, io,
):
    mr = lax.axis_index("row")
    mc = lax.axis_index("col")
    nch = nc // 2
    chip = mc // 2
    core = mc % 2
    partner = chip * 2 + (1 - core)
    slots, tile = tiles_in.shape[0], tiles_in.shape[1]
    mb, z = sino.shape
    nb = sol.shape[0]
    tr, tc = mb // tile, nb // tile
    sv, sr = nb // nr, mb // nc
    hz = z // 2

    inner = (mr == 1) | (mr == 2)
    outer = jnp.logical_not(inner)
    left = mr < 2
    mate = mr + 1 - 2 * lax.rem(mr, 2)
    cross = jnp.where(left, 2, 1)
    far = jnp.where(left, 3, 0)
    early = jnp.where(inner, far, mate)
    late = jnp.where(inner, mate, far)

    barrier = pltpu.get_barrier_semaphore()
    for s in range(1, nr):
        pl.semaphore_signal(barrier, 1, device_id=(lax.rem(mr + s, nr), mc), device_id_type=MESH)
    for s in range(1, nc):
        pl.semaphore_signal(barrier, 1, device_id=(mr, lax.rem(mc + s, nc)), device_id_type=MESH)
    load_sino = pltpu.make_async_copy(sino_in, sino, io.at[0])
    load_sino.start()
    load_tiles = []
    for i in range(4):
        some = pl.ds(slots // 4 * i, slots // 4)
        load_tiles.append(pltpu.make_async_copy(tiles_in.at[some], tiles.at[some], io.at[i + 2]))
        load_tiles[i].start()

    pending = {}

    def copy_to(src, dst, ssem, rsem, row, col):
        return pltpu.make_async_remote_copy(
            src_ref=src, dst_ref=dst, send_sem=ssem, recv_sem=rsem,
            device_id=(row, col), device_id_type=MESH)

    def settle(key):
        if key in pending:
            pending.pop(key).wait_send()

    def send(src, dst, ssems, rsems, h, s, slot, row, col):
        key = (id(ssems), h, s)
        settle(key)
        copy = copy_to(src, dst, ssems.at[h, s], rsems.at[h, slot], row, col)
        copy.start()
        pending[key] = copy
        return copy

    def chip_at(s):
        return (chip // 2 + s // 2) % 2 * 2 + (chip % 2 + s % 2) % 2

    def block(first, size):
        return pl.ds(pl.multiple_of(first, size), size)

    def pick(i, j):
        per = LANE // tc
        return tiles[inv[i // per, i % per * tc + j]]

    def column(row, h):
        return jnp.broadcast_to(row, (z, z)).T[h * hz:(h + 1) * hz]

    def wide(col, n):
        return jnp.concatenate([col] * (n // LANE), axis=1)

    def merge(a, b):
        lane = lax.broadcasted_iota(jnp.int32, (1, z), 1)
        return jnp.where(lane < hz, a, b)

    def share(vec, buf, n, me, ssems, rsems, kind, h, over_row):
        key = (id(ssems), kind, h)
        settle(key)
        buf[me] = jnp.broadcast_to(vec, (8, z))
        for s in range(1, n):
            peer = lax.rem(me + s, n)
            place = (peer, mc) if over_row else (mr, peer)
            copy_to(buf.at[me], buf.at[me], ssems.at[kind, h], rsems.at[kind, h], *place).start()
        others = buf.at[pl.ds(0, n - 1)]
        place = (lax.rem(mr + 1, nr), mc)
        pending[key] = copy_to(others, others, ssems.at[kind, h], rsems.at[kind, h], *place)

        def finish():
            copy_to(others, others, ssems.at[kind, h], rsems.at[kind, h], *place).wait_recv()
            total = buf[0]
            for q in range(1, n):
                total = total + buf[q]
            return total[:1]

        return finish

    def share_z(vec, n, h):
        return share(vec, zbuf.at[n, h], nr, mr, zs, zr, n % 2, h, True)

    def share_c(vec, n, h):
        return share(vec, cbuf.at[n, h], nc, mc, cs, cr, n % 2, h, False)

    def back_part(k, h, dest):
        cols = block(dest * sv, sv)
        if k == 0:
            if h == 0:
                build_fa(dest)
                val = dot(y0[...], fa[:, cols])
                bacc[1, dest] = val[hz:]
                return val[:hz]
            return bacc[1, dest]
        val = bacc[h, dest]
        q = chip_at(1) * 2
        for i in range(2):
            val = val + dot(yb[k, h, q + i], fa[block((q + i) * sr, sr), cols])
        return val

    def back_grow(k, h, q, fresh):
        for d in range(nr):
            cols = slice(d * sv, (d + 1) * sv)
            val = dot(yb[k, h, q], fa[block(q * sr, sr), cols])
            val = val + dot(yb[k, h, q + 1], fa[block((q + 1) * sr, sr), cols])
            bacc[h, d] = val if fresh else bacc[h, d] + val

    def back_start(k, h):
        col_pack(bsend.at[k, h, 0], back_part(k, h, jnp.where(inner, cross, far)))
        slot = jnp.where(inner, 3, 0)
        send(bsend.at[k, h, 0], brecv.at[k, h, slot], bs, br, h, 0, slot, jnp.where(inner, cross, mate), mc)
        settle((id(bs), h, 1))
        relay[h] = back_part(k, h, jnp.where(inner, far, cross))

        @pl.when(outer)
        def _():
            col_pack(bsend.at[k, h, 1], relay[h])
            copy_to(bsend.at[k, h, 1], brecv.at[k, h, 1], bs.at[h, 1], br.at[h, 1], cross, mc).start()

        col_pack(bsend.at[k, h, 2], back_part(k, h, mate))
        send(bsend.at[k, h, 2], brecv.at[k, h, 2], bs, br, h, 2, 2, mate, mc)
        vox[k, h] = back_part(k, h, mr)

    def back_arrived(k, h, slot):
        copy_to(bsend.at[k, h, slot], brecv.at[k, h, slot], bs.at[h, slot], br.at[h, slot], mate, mc).wait_recv()
        return col_unpack(brecv.at[k, h, slot], hz)

    def back_relay(k, h):
        @pl.when(inner)
        def _():
            col_pack(bsend.at[k, h, 1], relay[h] + back_arrived(k, h, 0))
            copy_to(bsend.at[k, h, 1], brecv.at[k, h, 1], bs.at[h, 1], br.at[h, 1], far, mc).start()

        pending[id(bs), h, 1] = copy_to(bsend.at[k, h, 1], brecv.at[k, h, 1], bs.at[h, 1], br.at[h, 1], mate, mc)

    def back_sum(k, h):
        @pl.when(inner)
        def _():
            vox[k, h] = vox[k, h] + back_arrived(k, h, 3)

        total = vox[k, h] + back_arrived(k, h, 2)
        return total + back_arrived(k, h, 1)

    def fwd_grow(k, h, origin, fresh):
        for q in range(nch):
            cols = slice(2 * q * sr, 2 * (q + 1) * sr)
            val = dot(xb[h, origin], ba[block(origin * sv, sv), cols])
            for i in range(2):
                half = val[:, i * sr:(i + 1) * sr]
                fpart[k, h, 2 * q + i] = half if fresh else fpart[k, h, 2 * q + i] + half

    def vox_take(k, h, origin):
        val = col_unpack(vgat.at[k, h, origin], hz)
        vfull[h, origin] = val
        xb[h, origin] = val.astype(jnp.bfloat16)

    def passed(k, h, origin, n, row):
        own = vgat.at[k, h, origin]
        return copy_to(own, own, vs.at[h, n], vr.at[h, origin], row, mc)

    def vox_send(k, h):
        @pl.when(inner)
        def _():
            if k:
                passed(k, h, mr, 2, far).wait_send()
                passed(k, h, far, 3, mate).wait_send()
            passed(k, h, mr, 2, far).start()

        own = vgat.at[k, h, mr]
        send(own, own, vs, vr, h, 1, mr, cross, mc)
        send(own, own, vs, vr, h, 0, mr, mate, mc)

    def vox_early(k, h):
        @pl.when(inner)
        def _():
            passed(k, h, far, 3, mate).wait_recv()
            passed(k, h, far, 3, mate).start()

        @pl.when(outer)
        def _():
            passed(k, h, mate, 0, mate).wait_recv()

        vox_take(k, h, early)

    def fwd_send(k, h):
        local = []
        for s in range(nch - 1, -1, -1):
            q = chip_at(s) * 2
            val = dot(xb[h, late], ba[block(late * sv, sv), block(q * sr, 2 * sr)])
            for i in range(2):
                fpart[k, h, q + i] = fpart[k, h, q + i] + val[:, i * sr:(i + 1) * sr]
            local.append(send(fpart.at[k, h, q + 1 - core], drecv.at[k, h, s], ds_, dr, h, s, s, mr, partner))
        return local

    def fwd_pass(k, h, local):
        copies = []
        for s, other in zip(range(nch - 1, -1, -1), local):
            q = chip_at(s) * 2 + core
            other.wait_recv()
            part = fpart[k, h, q] + drecv[k, h, s]
            if s:
                col_pack(fsend.at[k, h, s], part)
                copies.append(send(fsend.at[k, h, s], frecv.at[k, h, s], fs, fr, h, s, s, mr, q))
            else:
                ray[k + 1, h] = part
        return copies

    def fwd_sum(k, h, copies):
        total = ray[k + 1, h]
        for i, copy in enumerate(copies):
            copy.wait_recv()
            total = total + col_unpack(frecv.at[k, h, nch - 1 - i], hz)
        return total

    def flip(first, last):
        @pl.loop(first, last)
        def _(d):
            for j in range(sv // LANE):
                cols = slice(j * LANE, (j + 1) * LANE)
                both = jnp.concatenate([vfull[0, d, :, cols], vfull[1, d, :, cols]], axis=0)
                vrow[block(d * sv + j * LANE, LANE), :] = both.T

    alphas = [[None, None] for _ in range(ITERS)]
    betas = [[None, None] for _ in range(ITERS + 1)]
    run = {}

    def update_dir(k):
        alpha = merge(*alphas[k])
        inv_alpha = 1.0 / alpha
        if k == 0:
            run["rho_bar"] = alpha
            sdir[...] = vrow[...] * inv_alpha
        else:
            theta = run["sine"] * alpha
            run["rho_bar"] = -run["cosine"] * alpha
            sdir[...] = vrow[...] * inv_alpha - (theta / run["rho"]) * sdir[...]

    def update_sol(k):
        beta = merge(*betas[k + 1])
        rho_bar = run["rho_bar"]
        rho = jnp.sqrt(rho_bar * rho_bar + beta * beta)
        run["rho"] = rho
        run["cosine"] = rho_bar / rho
        run["sine"] = beta / rho
        phi = run["cosine"] * run["phi_bar"]
        run["phi_bar"] = run["sine"] * run["phi_bar"]
        if k + 1 == ITERS:
            res[0:8] = jnp.broadcast_to(phi / rho, (8, z))
            res[8:16] = jnp.broadcast_to(run["phi_bar"], (8, z))
            return
        step = (phi / rho) * sdir[...]
        sol[...] = step if k == 0 else sol[...] + step

    def half(h):
        beta_of = None
        for k in range(ITERS):
            back_start(k, h)
            if k == 0 and h:
                build_ba(mr)
            yield
            back_relay(k, h)
            if k == 0:
                build_ba(cross if h else early)
            yield
            if k == 0 and h:
                build_ba(late)
            total = back_sum(k, h)
            if k:
                betas[k][h] = root(beta_of)
            elif not h:
                run["phi_bar"] = root(first_norm)
                betas[0] = [run["phi_bar"], run["phi_bar"]]
            beta = betas[k][h]
            raw = total * wide(column(1.0 / beta, h), sv)
            if k:
                raw = raw - wide(column(beta / alphas[k - 1][h], h), sv) * vox[k - 1, h]
            vox[k, h] = raw
            col_pack(vgat.at[k, h, mr], raw)
            vox_send(k, h)
            alpha_of = share_z(row_squares(raw), 2 * k + 1, h)
            vox_take(k, h, mr)
            fwd_grow(k, h, mr, True)
            if k and h:
                update_sol(k - 1)
            yield
            vox_early(k, h)
            fwd_grow(k, h, early, False)
            yield
            passed(k, h, cross, 0, mate).wait_recv()
            vox_take(k, h, cross)
            fwd_grow(k, h, cross, False)
            yield
            passed(k, h, late, 0, mate).wait_recv()
            vox_take(k, h, late)
            local = fwd_send(k, h)
            alpha_of = share_c(alpha_of(), 2 * k + 1, h)
            yield
            copies = fwd_pass(k, h, local)
            if h:
                flip(0, nr)
            yield
            total = fwd_sum(k, h, copies)
            alpha = root(alpha_of)
            alphas[k][h] = alpha
            raw = total * wide(column(1.0 / alpha, h), sr)
            raw = raw - wide(column(alpha / beta, h), sr) * ray[k, h]
            n = 2 * k + 2
            if k + 1 == ITERS:
                beta_of = share_c(row_squares(raw), n, h)
                if h:
                    update_dir(k)
                yield
                beta_of = share_z(beta_of(), n, h)
                yield
                betas[k + 1][h] = root(beta_of)
                return
            ray[k + 1, h] = raw
            own = yb.at[k + 1, h, mc]
            own[...] = raw.astype(jnp.bfloat16)
            across = [send(own, own, gs, gr, h, 0, 0, mr, partner)]
            for s in range(nch - 1, 0, -1):
                across.append(send(own, own, gs, gr, h, s, s, mr, chip_at(s) * 2 + core))
            beta_of = share_c(row_squares(raw), n, h)
            if h:
                update_dir(k)
            yield
            across[0].wait_recv()
            back_grow(k + 1, h, chip * 2, True)
            yield
            hand = []
            for s in range(nch - 1, 0, -1):
                across[nch - s].wait_recv()
                origin = chip_at(s) * 2 + core
                given = yb.at[k + 1, h, origin]
                hand.append(send(given, given, hs, hr, h, s, s, mr, partner))
            beta_of = share_z(beta_of(), n, h)
            yield
            for s in range(nch - 1, 0, -1):
                hand[nch - 1 - s].wait_recv()
                if s > 1:
                    back_grow(k + 1, h, chip_at(s) * 2, False)

    def build_fa(dest):
        wide_by = sv // tile

        @pl.loop(0, tr)
        def _(i):
            for j in range(wide_by):
                fa[block(i * tile, tile), block(dest * sv + j * tile, tile)] = pick(i, dest * wide_by + j)

    def build_ba(origin):
        wide_by = sv // tile

        @pl.loop(0, wide_by)
        def _(j):
            for i in range(tr):
                ba[block(origin * sv + j * tile, tile), i * tile:(i + 1) * tile] = pick(i, origin * wide_by + j).T

    place = jnp.broadcast_to(place_of[...], (LANE, slots)).T
    slot_of = lax.broadcasted_iota(jnp.int32, (slots, LANE), 0)
    for i in range(inv.shape[0]):
        spot = lax.broadcasted_iota(jnp.int32, (slots, LANE), 1) + i * LANE
        inv_row[i:i + 1, :] = jnp.min(jnp.where(place == spot, slot_of, slots), axis=0, keepdims=True)
    move = pltpu.make_async_copy(inv_row, inv, io.at[1])
    move.start()
    tiles[slots] = jnp.zeros((tile, tile), tiles.dtype)
    load_sino.wait()
    total = squares(sino[...])
    for i in range(tr):
        y0[:, i * tile:(i + 1) * tile] = sino[i * tile:(i + 1) * tile, :].T.astype(jnp.bfloat16)
    own = sino[block(mc * sr, sr), :].T
    ray[0, 0] = own[:hz]
    ray[0, 1] = own[hz:]
    move.wait()
    for load in load_tiles:
        load.wait()

    pl.semaphore_wait(barrier, nr - 1 + nc - 1)
    first_norm = share_z(total, 0, 0)
    halves = [half(0), half(1)]
    for h in ORDER:
        next(halves[h], None)
    update_sol(ITERS - 1)
    for key in list(pending):
        settle(key)

    @pl.when(inner)
    def _():
        for h in range(2):
            passed(0, h, mr, 2, far).wait_send()
            passed(0, h, far, 3, mate).wait_send()


def finish_kernel(x, d, scale, out, last, val, sems):
    parts = sems.shape[0]
    n = x.shape[0] // parts
    last[...] = scale[8:9, :]
    stores = []
    for i in range(parts):
        rows = pl.ds(i * n, n)
        val[rows, :] = x[rows, :] + scale[0:1, :] * d[rows, :]
        stores.append(pltpu.make_async_copy(val.at[rows], out.at[rows], sems.at[i]))
        stores[i].start()
    for store in stores:
        store.wait()


def body(nr, nc, tile_values, tile_rows, tile_cols, tile_count, sinogram):
    values = tile_values[0, 0]
    slots, tile = values.shape[0], values.shape[1]
    mb, z = sinogram.shape
    nb = TC * tile
    tr = mb // tile
    sv, sr = nb // nr, mb // nc
    if nr != 4 or nc != 8 or sr % LANE or sv % LANE or z != LANE:
        return body_rows(nr, nc, tile_values, tile_rows, tile_cols, tile_count, sinogram)
    ids = jnp.arange(slots, dtype=jnp.int32)[None, :]
    place = jnp.where(ids < tile_count, tile_rows[0] * TC + tile_cols[0], -1)
    nch, hz = nc // 2, z // 2
    f32, bf16, i16 = jnp.float32, jnp.bfloat16, jnp.int16
    dma, vmem_of = pltpu.SemaphoreType.DMA, pltpu.VMEM
    vmem = pl.BlockSpec(memory_space=pltpu.VMEM)
    hbm = pl.BlockSpec(memory_space=pltpu.HBM)
    pb, pf = sv // LANE * hz + PAD, sr // LANE * hz + PAD
    norms = 2 * ITERS + 1
    spots = tr * TC // LANE
    scratch = [
        vmem_of((slots + 1, tile, tile), bf16), vmem_of((mb, z), f32),
        vmem_of((spots, LANE), jnp.int32), pltpu.SMEM((spots, LANE), jnp.int32),
        vmem_of((mb, nb), bf16), vmem_of((nb, mb), bf16), vmem_of((z, mb), bf16),
        vmem_of((ITERS, 2, nc, hz, sr), bf16), vmem_of((2, nr, hz, sv), f32),
        vmem_of((ITERS, 2, nc, hz, sr), f32), vmem_of((ITERS, 2, nch, hz, sr), f32),
        vmem_of((2, nr, hz, sv), bf16), vmem_of((2, nr, hz, sv), f32),
        vmem_of((ITERS + 1, 2, hz, sr), f32), vmem_of((ITERS, 2, hz, sv), f32), vmem_of((2, hz, sv), f32),
        vmem_of((nb, z), f32),
        vmem_of((ITERS, 2, nr, pb, LANE), i16), vmem_of((ITERS, 2, nr, pb, LANE), i16),
        vmem_of((ITERS, 2, nr, pb, LANE), i16),
        vmem_of((ITERS, 2, nch, pf, LANE), i16), vmem_of((ITERS, 2, nch, pf, LANE), i16),
        vmem_of((norms, 2, nr, 8, z), f32), vmem_of((norms, 2, nc, 8, z), f32),
    ] + [dma((2, nr))] * 4 + [dma((2, nch))] * 8 + [dma((2, 2))] * 4 + [dma((6,))]
    part = jax.ShapeDtypeStruct((nb, z), f32)
    sol, step, scale = pl.pallas_call(
        functools.partial(kernel, nr, nc),
        out_shape=(part, part, jax.ShapeDtypeStruct((16, z), f32)),
        in_specs=[vmem, hbm, hbm],
        out_specs=(vmem, vmem, vmem),
        scratch_shapes=scratch,
        compiler_params=pltpu.CompilerParams(
            collective_id=0, has_side_effects=True, vmem_limit_bytes=GRANT),
    )(place, values, sinogram)
    sol, last = pl.pallas_call(
        finish_kernel,
        out_shape=(part, jax.ShapeDtypeStruct((1, z), f32)),
        in_specs=[vmem, vmem, vmem],
        out_specs=(hbm, vmem),
        scratch_shapes=[vmem_of((nb, z), f32), dma((4,))],
        compiler_params=pltpu.CompilerParams(vmem_limit_bytes=8 * 1024 * 1024),
    )(sol, step, scale)
    return sol, last[0]


def solution(mesh):
    nr, nc = mesh.shape["row"], mesh.shape["col"]
    in_specs = (
        P("row", "col", None, None, None),
        P("row", "col", None),
        P("row", "col", None),
        P("row", "col"),
        P("row", None),
    )
    return jax.shard_map(
        functools.partial(body, nr, nc), mesh=mesh, in_specs=in_specs,
        out_specs=(P("col", None), P()), check_vma=False)
```

```python
import functools

import jax
import jax.numpy as jnp
from jax import lax
from jax.experimental import pallas as pl
from jax.experimental.pallas import tpu as pltpu
from jax.sharding import PartitionSpec as P

TC = 16
ITERS = 3
EPSILON = 1e-06
PAD = 16
TOP = 32000.0
FINE = 64.0
LANE = 128
GRANT = 53000 * 1024
ORDER = [int(one) for one in '0001001001001101010110110010010011010101101100100101111101']
MESH = pl.DeviceIdType.MESH


def pack(val):
    top = jnp.max(jnp.abs(val), axis=0, keepdims=True)
    exponent = jnp.ceil(jnp.log2(jnp.maximum(top, 1e-30)))
    scale = TOP * jnp.exp2(-exponent)
    coded = jnp.round(jnp.clip(val * scale, -32767.0, 32767.0))
    coded = coded.astype(jnp.int32).astype(jnp.int16)
    rows = jnp.broadcast_to(exponent, (PAD, val.shape[1]))
    return coded, rows.astype(jnp.int32).astype(jnp.int16)


def store_packet(ref, val):
    n = val.shape[0]
    coded, rows = pack(val)
    ref[pl.ds(0, n), :] = coded
    ref[pl.ds(n, PAD), :] = rows


def load_packet(ref):
    n = ref.shape[0] - PAD
    exponent = ref[pl.ds(n, PAD), :].astype(jnp.int32).astype(jnp.float32)[:1]
    scale = jnp.exp2(exponent) * (1.0 / TOP)
    return ref[pl.ds(0, n), :].astype(jnp.int32).astype(jnp.float32) * scale


def dot(a, b):
    return jnp.dot(a, b, preferred_element_type=jnp.float32)


def root(total_of):
    return jnp.sqrt(total_of() + EPSILON)


def squares(vec):
    return jnp.sum(vec * vec, axis=0, keepdims=True)


def kernel_rows(
    nr, nc, inv, tiles, sino, sol, res,
    facc, bacc, sq, fa, ba, ybf, xbf, ray, vox, vfull, sdir,
    bsend, brecv, vgat, dsend, drecv, fsend, frecv, rgat, nrow, ncol, nlast,
    bs, br, vs, vr, ds_, dr, fs, fr, gs, gr, hs, hr, rs, rr, cs, cr, ls, lr,
):
    mr = lax.axis_index("row")
    mc = lax.axis_index("col")
    nch = nc // 2
    chip = mc // 2
    core = mc % 2
    partner = chip * 2 + (1 - core)
    tile = tiles.shape[1]
    mb, z = sino.shape
    nb = sol.shape[0]
    tr, tc = mb // tile, nb // tile
    sv, sr = nb // nr, mb // nc

    barrier = pltpu.get_barrier_semaphore()
    for s in range(1, nr):
        pl.semaphore_signal(barrier, 1, device_id=(lax.rem(mr + s, nr), mc), device_id_type=MESH)
    for s in range(1, nc):
        pl.semaphore_signal(barrier, 1, device_id=(mr, lax.rem(mc + s, nc)), device_id_type=MESH)

    def send(src, dst, ssem, rsem, row, col):
        copy = pltpu.make_async_remote_copy(
            src_ref=src, dst_ref=dst, send_sem=ssem, recv_sem=rsem,
            device_id=(row, col), device_id_type=MESH)
        copy.start()
        sent.append(copy)
        return copy

    sent = []

    def pick(i, j):
        slot = inv[i * tc + j]
        block = tiles[jnp.maximum(slot, 0)]
        return jnp.where(slot >= 0, block, jnp.zeros_like(block))

    @pl.loop(0, tc)
    def _(j):
        first = pl.multiple_of(j * tile, tile)
        for i in range(tr):
            ba[pl.ds(first, tile), i * tile:(i + 1) * tile] = pick(i, j).T

    def share(vec, buf, n, me, ssem, rsem, over_row):
        buf[me] = jnp.broadcast_to(vec, (8, z))
        copies = []
        for s in range(1, n):
            peer = lax.rem(me + s, n)
            place = (peer, mc) if over_row else (mr, peer)
            copies.append(send(buf.at[me], buf.at[me], ssem.at[s], rsem.at[s], *place))

        def finish():
            for copy in copies:
                copy.wait_recv()
            total = buf[0]
            for q in range(1, n):
                total = total + buf[q]
            return total[:1]

        return finish

    line = nr == 4
    inner = (mr == 1) | (mr == 2)
    left = mr < 2
    mate = mr + 1 - 2 * lax.rem(mr, 2)
    cross = jnp.where(left, 2, 1)
    far = jnp.where(left, 3, 0)
    early = jnp.where(inner, far, mate)
    late = jnp.where(inner, mate, far)
    inner_sent = []

    def row_copy(src, dst, ssem, rsem, row):
        return pltpu.make_async_remote_copy(
            src_ref=src, dst_ref=dst, send_sem=ssem, recv_sem=rsem,
            device_id=(row, mc), device_id_type=MESH)

    def back_part(k, dest):
        rows = pl.ds(pl.multiple_of(dest * sv, sv), sv)
        if k == 0:
            return dot(ba[rows, :], ybf[...])
        late = lax.rem(chip + 1, nch) * 2 * sr
        cols = pl.ds(pl.multiple_of(late, 2 * sr), 2 * sr)
        return bacc[rows, :] + dot(ba[rows, cols], ybf[cols, :])

    def back_arrived(k, slot):
        row_copy(bsend.at[k, slot], brecv.at[k, slot], bs.at[k, slot], br.at[k, slot], mate).wait_recv()

    def back_start(k):
        if line:
            store_packet(bsend.at[k, 0], back_part(k, jnp.where(inner, cross, far)))
            slot = jnp.where(inner, 3, 0)
            send(bsend.at[k, 0], brecv.at[k, slot], bs.at[k, 0], br.at[k, slot],
                 jnp.where(inner, cross, mate), mc)
            part = back_part(k, jnp.where(inner, far, cross))

            @pl.when(jnp.logical_not(inner))
            def _():
                store_packet(bsend.at[k, 1], part)

            @pl.when(inner)
            def _():
                back_arrived(k, 0)
                store_packet(bsend.at[k, 1], part + load_packet(brecv.at[k, 0]))

            send(bsend.at[k, 1], brecv.at[k, 1], bs.at[k, 1], br.at[k, 1], jnp.where(inner, far, cross), mc)
            store_packet(bsend.at[k, 2], back_part(k, mate))
            send(bsend.at[k, 2], brecv.at[k, 2], bs.at[k, 2], br.at[k, 2], mate, mc)
            vox[k] = back_part(k, mr)
            return None
        copies = []
        for s in list(range(1, nr)) + [0]:
            dest = lax.rem(mr + s, nr)
            part = back_part(k, dest)
            if s:
                store_packet(bsend.at[k, s], part)
                copies.append(send(bsend.at[k, s], brecv.at[k, s], bs.at[k, s], br.at[k, s], dest, mc))
            else:
                vox[k] = part
        return copies

    def back_sum(k, copies):
        if line:
            @pl.when(inner)
            def _():
                back_arrived(k, 3)
                vox[k] = vox[k] + load_packet(brecv.at[k, 3])

            total = vox[k]
            for slot in (2, 1):
                back_arrived(k, slot)
                total = total + load_packet(brecv.at[k, slot])
            return total
        total = vox[k]
        for i, copy in enumerate(copies):
            copy.wait_recv()
            total = total + load_packet(brecv.at[k, i + 1])
        return total

    def vox_take(k, origin):
        val = load_packet(vgat.at[k, origin])
        rows = pl.ds(pl.multiple_of(origin * sv, sv), sv)
        vfull[rows, :] = val
        xbf[rows, :] = val.astype(jnp.bfloat16)

    def grow(acc, mat, vec, first, depth, fresh):
        cols = pl.ds(pl.multiple_of(first, depth), depth)

        @pl.loop(0, acc.shape[0] // sv)
        def _(i):
            rows = pl.ds(pl.multiple_of(i * sv, sv), sv)
            val = dot(mat[rows, cols], vec[cols, :])
            acc[rows, :] = val if fresh else acc[rows, :] + val

    def vox_gather(k):
        store_packet(vgat.at[k, mr], vox[k])
        if line:
            def passed(origin, n, row):
                return row_copy(vgat.at[k, origin], vgat.at[k, origin], vs.at[k, n], vr.at[k, origin], row)

            @pl.when(inner)
            def _():
                passed(mr, 2, far).start()

            send(vgat.at[k, mr], vgat.at[k, mr], vs.at[k, 1], vr.at[k, mr], cross, mc)
            send(vgat.at[k, mr], vgat.at[k, mr], vs.at[k, 0], vr.at[k, mr], mate, mc)
            inner_sent.append(passed(mr, 2, far))
            inner_sent.append(passed(far, 3, mate))
            vox_take(k, mr)
            grow(facc, fa, xbf, mr * sv, sv, True)

            @pl.when(inner)
            def _():
                passed(far, 3, mate).wait_recv()
                passed(far, 3, mate).start()

            @pl.when(jnp.logical_not(inner))
            def _():
                passed(mate, 0, mate).wait_recv()

            vox_take(k, early)
            grow(facc, fa, xbf, early * sv, sv, False)
            passed(cross, 0, mate).wait_recv()
            vox_take(k, cross)
            grow(facc, fa, xbf, cross * sv, sv, False)
            passed(late, 0, mate).wait_recv()
            vox_take(k, late)
        else:
            copies = [
                send(vgat.at[k, mr], vgat.at[k, mr], vs.at[k, s], vr.at[k, s], lax.rem(mr + s, nr), mc)
                for s in range(1, nr)
            ]
            for copy in copies:
                copy.wait_recv()
            for q in range(nr):
                vox_take(k, q)
        return share(squares(vfull[...]), ncol.at[k], nc, mc, cs.at[k], cr.at[k], False)

    def fwd_part(first):
        rows = pl.ds(first, sr)
        if line:
            cols = pl.ds(pl.multiple_of(late * sv, sv), sv)
            return facc[rows, :] + dot(fa[rows, cols], xbf[cols, :])
        return dot(fa[rows, :], xbf[...])

    def fwd_start(k):
        order = list(range(1, nch)) + [0]
        local = []
        for s in order:
            q = lax.rem(chip + s, nch)
            first = pl.multiple_of((q * 2 + 1 - core) * sr, sr)
            dsend[k, s] = fwd_part(first)
            local.append(send(dsend.at[k, s], drecv.at[k, s], ds_.at[k, s], dr.at[k, s], mr, partner))
        copies = []
        for s, other in zip(order, local):
            q = lax.rem(chip + s, nch)
            first = pl.multiple_of((q * 2 + core) * sr, sr)
            part = fwd_part(first)
            other.wait_recv()
            part = part + drecv[k, s]
            if s:
                store_packet(fsend.at[k, s], part)
                copies.append(send(fsend.at[k, s], frecv.at[k, s], fs.at[k, s], fr.at[k, s], mr, q * 2 + core))
            else:
                ray[k + 1] = part
        return copies

    def fwd_sum(k, copies):
        total = ray[k + 1]
        for i, copy in enumerate(copies):
            copy.wait_recv()
            total = total + load_packet(frecv.at[k, i + 1])
        return total

    def ray_gather(k):
        store_packet(rgat.at[k, mc], ray[k + 1])
        across = [send(rgat.at[k, mc], rgat.at[k, mc], gs.at[k, 0], gr.at[k, 0], mr, partner)]
        for s in range(1, nch):
            peer = lax.rem(chip + s, nch) * 2 + core
            across.append(send(rgat.at[k, mc], rgat.at[k, mc], gs.at[k, s], gr.at[k, s], mr, peer))
        hand = [None]

        def take(origin):
            val = load_packet(rgat.at[k, origin])
            sq[origin] = jnp.broadcast_to(squares(val), (8, z))
            ybf[pl.ds(pl.multiple_of(origin * sr, sr), sr), :] = val.astype(jnp.bfloat16)

        take(mc)
        across[0].wait_recv()
        take(partner)
        grow(bacc, ba, ybf, chip * 2 * sr, 2 * sr, True)
        for s in range(1, nch):
            across[s].wait_recv()
            origin = lax.rem(chip + nch - s, nch) * 2 + core
            hand.append(send(rgat.at[k, origin], rgat.at[k, origin], hs.at[k, s], hr.at[k, s], mr, partner))
            take(origin)
        for s in range(1, nch):
            hand[s].wait_recv()
            origin = lax.rem(chip + nch - s, nch) * 2
            take(origin + 1 - core)
            if s + 1 < nch:
                grow(bacc, ba, ybf, origin * sr, 2 * sr, False)
        total = jnp.zeros((1, z), jnp.float32)
        for q in range(nc):
            total = total + sq[q][:1]
        return share(total, nrow.at[k + 1], nr, mr, rs.at[k + 1], rr.at[k + 1], True)

    ybf[...] = sino[...].astype(jnp.bfloat16)
    total = squares(sino[...])
    pl.semaphore_wait(barrier, nr - 1 + nc - 1)
    beta_of = share(total, nrow.at[0], nr, mr, rs.at[0], rr.at[0], True)
    copies = back_start(0)

    @pl.loop(0, tr)
    def _(i):
        first = pl.multiple_of(i * tile, tile)
        for j in range(tc):
            fa[pl.ds(first, tile), j * tile:(j + 1) * tile] = pick(i, j)

    beta = root(beta_of)
    ray[0] = sino[pl.ds(pl.multiple_of(mc * sr, sr), sr), :] * (1.0 / beta)
    vox[0] = back_sum(0, copies) * (1.0 / beta)
    alpha_of = vox_gather(0)
    phi_bar = beta
    for k in range(ITERS):
        copies = fwd_start(k)
        alpha = root(alpha_of)
        inv_alpha = 1.0 / alpha
        if k == 0:
            rho_bar = alpha
            sdir[...] = vfull[...] * inv_alpha
        else:
            theta = sine * alpha
            rho_bar = -cosine * alpha
            sdir[...] = vfull[...] * inv_alpha - (theta / rho) * sdir[...]
        vox[k] = vox[k] * inv_alpha
        ray_raw = fwd_sum(k, copies) * inv_alpha - alpha * ray[k]
        last = k + 1 == ITERS
        if last:
            total = share(squares(ray_raw), nlast, nc, mc, ls, lr, False)()
            beta = root(share(total, nrow.at[k + 1], nr, mr, rs.at[k + 1], rr.at[k + 1], True))
        else:
            ray[k + 1] = ray_raw
            beta_of = ray_gather(k)
            copies = back_start(k + 1)
            beta = root(beta_of)
            ray[k + 1] = ray[k + 1] * (1.0 / beta)
        rho = jnp.sqrt(rho_bar * rho_bar + beta * beta)
        cosine = rho_bar / rho
        sine = beta / rho
        phi = cosine * phi_bar
        phi_bar = sine * phi_bar
        step = (phi / rho) * sdir[...]
        sol[...] = step if k == 0 else sol[...] + step
        if not last:
            vox[k + 1] = back_sum(k + 1, copies) * (1.0 / beta) - beta * vox[k]
            alpha_of = vox_gather(k + 1)
    res[...] = jnp.broadcast_to(phi_bar, res.shape)
    for copy in sent:
        copy.wait_send()
    if line:
        @pl.when(inner)
        def _():
            for copy in inner_sent:
                copy.wait_send()


def body_rows(nr, nc, tile_values, tile_rows, tile_cols, tile_count, sinogram):
    values = tile_values[0, 0]
    slots, tile = values.shape[0], values.shape[1]
    mb, z = sinogram.shape
    nb = TC * tile
    tr = mb // tile
    place = tile_rows[0, 0] * TC + tile_cols[0, 0]
    ids = jnp.arange(slots, dtype=jnp.int32)
    place = jnp.where(ids < tile_count[0, 0], place, -1)
    hit = place[None, :] == jnp.arange(tr * TC, dtype=jnp.int32)[:, None]
    inv = jnp.sum(jnp.where(hit, ids[None, :] + 1, 0), axis=1, dtype=jnp.int32) - 1
    nch = nc // 2
    sv, sr = nb // nr, mb // nc
    f32, bf16, i16 = jnp.float32, jnp.bfloat16, jnp.int16
    dma = pltpu.SemaphoreType.DMA
    vmem = pl.BlockSpec(memory_space=pltpu.VMEM)
    scratch = [
        pltpu.VMEM((mb, z), f32), pltpu.VMEM((nb, z), f32), pltpu.VMEM((nc, 8, z), f32),
        pltpu.VMEM((mb, nb), bf16), pltpu.VMEM((nb, mb), bf16),
        pltpu.VMEM((mb, z), bf16), pltpu.VMEM((nb, z), bf16),
        pltpu.VMEM((ITERS + 1, sr, z), f32), pltpu.VMEM((ITERS, sv, z), f32),
        pltpu.VMEM((nb, z), f32), pltpu.VMEM((nb, z), f32),
        pltpu.VMEM((ITERS, nr, sv + PAD, z), i16), pltpu.VMEM((ITERS, nr, sv + PAD, z), i16),
        pltpu.VMEM((ITERS, nr, sv + PAD, z), i16),
        pltpu.VMEM((ITERS, nch, sr, z), f32), pltpu.VMEM((ITERS, nch, sr, z), f32),
        pltpu.VMEM((ITERS, nch, sr + PAD, z), i16), pltpu.VMEM((ITERS, nch, sr + PAD, z), i16),
        pltpu.VMEM((ITERS, nc, sr + PAD, z), i16),
        pltpu.VMEM((ITERS + 1, nr, 8, z), f32), pltpu.VMEM((ITERS, nc, 8, z), f32),
        pltpu.VMEM((nc, 8, z), f32),
        dma((ITERS, nr)), dma((ITERS, nr)), dma((ITERS, nr)), dma((ITERS, nr)),
        dma((ITERS, nch)), dma((ITERS, nch)), dma((ITERS, nch)), dma((ITERS, nch)),
        dma((ITERS, nch)), dma((ITERS, nch)), dma((ITERS, nch)), dma((ITERS, nch)),
        dma((ITERS + 1, nr)), dma((ITERS + 1, nr)), dma((ITERS, nc)), dma((ITERS, nc)),
        dma((nc,)), dma((nc,)),
    ]
    sol, res = pl.pallas_call(
        functools.partial(kernel_rows, nr, nc),
        out_shape=(jax.ShapeDtypeStruct((nb, z), f32), jax.ShapeDtypeStruct((8, z), f32)),
        in_specs=[pl.BlockSpec(memory_space=pltpu.SMEM), vmem, vmem],
        out_specs=(vmem, vmem),
        scratch_shapes=scratch,
        compiler_params=pltpu.CompilerParams(
            collective_id=0, has_side_effects=True, vmem_limit_bytes=60 * 1024 * 1024),
    )(inv, values, sinogram)
    return sol, res[0]


def col_pack(ref, val):
    h, n = val.shape
    groups = h // PAD
    mag = jnp.abs(val)
    top = mag[:PAD]
    for g in range(1, groups):
        top = jnp.maximum(top, mag[g * PAD:(g + 1) * PAD])
    top = jnp.max(top, axis=1, keepdims=True)
    exponent = jnp.ceil(jnp.log2(jnp.maximum(top, 1e-30)) * FINE)
    scale = jnp.concatenate([TOP * jnp.exp2(exponent * (-1.0 / FINE))] * groups, axis=0)
    coded = jnp.round(val * scale).astype(jnp.int32).astype(jnp.int16)
    for j in range(n // LANE):
        ref[pl.ds(j * h, h), :] = coded[:, j * LANE:(j + 1) * LANE]
    ref[pl.ds(n // LANE * h, PAD), :] = jnp.broadcast_to(exponent, (PAD, LANE)).astype(jnp.int32).astype(jnp.int16)


def col_unpack(ref, h):
    blocks = (ref.shape[0] - PAD) // h
    exponent = ref[pl.ds(blocks * h, PAD), :].astype(jnp.int32).astype(jnp.float32)
    scale = jnp.concatenate([jnp.exp2(exponent * (1.0 / FINE)) * (1.0 / TOP)] * (h // PAD), axis=0)
    return jnp.concatenate(
        [ref[pl.ds(j * h, h), :].astype(jnp.int32).astype(jnp.float32) * scale for j in range(blocks)], axis=1)


def row_squares(val):
    h, n = val.shape
    acc = jnp.zeros((h, LANE), jnp.float32)
    for j in range(n // LANE):
        part = val[:, j * LANE:(j + 1) * LANE]
        acc = acc + part * part
    acc = jnp.concatenate([acc] * (LANE // h), axis=0)
    return jnp.sum(acc.T, axis=0, keepdims=True)


def kernel(
    nr, nc, place_of, tiles_in, sino_in, sol, sdir, res,
    tiles, sino, inv_row, inv,
    fa, ba, y0, yb, bacc, fpart, drecv, xb, vfull, ray, vox, relay, vrow,
    bsend, brecv, vgat, fsend, frecv, zbuf, cbuf, abuf,
    bs, br, vs, vr, ds_, dr, fs, fr, gs, gr, hs, hr, zs, zr, cs, cr, as_, ar, io,
):
    mr = lax.axis_index("row")
    mc = lax.axis_index("col")
    nch = nc // 2
    chip = mc // 2
    core = mc % 2
    partner = chip * 2 + (1 - core)
    slots, tile = tiles_in.shape[0], tiles_in.shape[1]
    mb, z = sino.shape
    nb = sol.shape[0]
    tr, tc = mb // tile, nb // tile
    sv, sr = nb // nr, mb // nc
    hz = z // 2

    inner = (mr == 1) | (mr == 2)
    outer = jnp.logical_not(inner)
    left = mr < 2
    mate = mr + 1 - 2 * lax.rem(mr, 2)
    cross = jnp.where(left, 2, 1)
    far = jnp.where(left, 3, 0)
    early = jnp.where(inner, far, mate)
    late = jnp.where(inner, mate, far)

    barrier = pltpu.get_barrier_semaphore()
    for r in range(nr):
        for c in range(nc):
            if r or c:
                pl.semaphore_signal(
                    barrier, 1, device_id=(lax.rem(mr + r, nr), lax.rem(mc + c, nc)), device_id_type=MESH)
    load_sino = pltpu.make_async_copy(sino_in, sino, io.at[0])
    load_sino.start()
    load_tiles = []
    for i in range(4):
        some = pl.ds(slots // 4 * i, slots // 4)
        load_tiles.append(pltpu.make_async_copy(tiles_in.at[some], tiles.at[some], io.at[i + 2]))
        load_tiles[i].start()

    pending = {}

    def copy_to(src, dst, ssem, rsem, row, col):
        return pltpu.make_async_remote_copy(
            src_ref=src, dst_ref=dst, send_sem=ssem, recv_sem=rsem,
            device_id=(row, col), device_id_type=MESH)

    def settle(key):
        if key in pending:
            pending.pop(key).wait_send()

    def send(src, dst, ssems, rsems, h, s, slot, row, col):
        key = (id(ssems), h, s)
        settle(key)
        copy = copy_to(src, dst, ssems.at[h, s], rsems.at[h, slot], row, col)
        copy.start()
        pending[key] = copy
        return copy

    def chip_at(s):
        return (chip // 2 + s // 2) % 2 * 2 + (chip % 2 + s % 2) % 2

    def block(first, size):
        return pl.ds(pl.multiple_of(first, size), size)

    def pick(i, j):
        per = LANE // tc
        return tiles[inv[i // per, i % per * tc + j]]

    def column(row, h):
        return jnp.broadcast_to(row, (z, z)).T[h * hz:(h + 1) * hz]

    def wide(col, n):
        return jnp.concatenate([col] * (n // LANE), axis=1)

    def merge(a, b):
        lane = lax.broadcasted_iota(jnp.int32, (1, z), 1)
        return jnp.where(lane < hz, a, b)

    def share(vec, buf, n, me, ssems, rsems, kind, h, over_row):
        key = (id(ssems), kind, h)
        settle(key)
        buf[me] = jnp.broadcast_to(vec, (8, z))
        for s in range(1, n):
            peer = lax.rem(me + s, n)
            place = (peer, mc) if over_row else (mr, peer)
            copy_to(buf.at[me], buf.at[me], ssems.at[kind, h], rsems.at[kind, h], *place).start()
        others = buf.at[pl.ds(0, n - 1)]
        place = (lax.rem(mr + 1, nr), mc)
        pending[key] = copy_to(others, others, ssems.at[kind, h], rsems.at[kind, h], *place)

        def finish():
            copy_to(others, others, ssems.at[kind, h], rsems.at[kind, h], *place).wait_recv()
            total = buf[0]
            for q in range(1, n):
                total = total + buf[q]
            return total[:1]

        return finish

    def share_all(vec, h):
        buf, me = abuf.at[h], mr * nc + mc
        buf[me] = vec
        for r in range(nr):
            for c in range(nc):
                if r or c:
                    copy_to(buf.at[me], buf.at[me], as_.at[h], ar.at[h],
                            lax.rem(mr + r, nr), lax.rem(mc + c, nc)).start()
        others = buf.at[pl.ds(0, nr * nc - 1)]
        arrived = copy_to(others, others, as_.at[h], ar.at[h], lax.rem(mr + 1, nr), mc)
        pending[id(as_), h] = arrived

        def finish():
            arrived.wait_recv()
            total = buf[0]
            for q in range(1, nr * nc):
                total = total + buf[q]
            return total

        return finish

    def share_z(vec, n, h):
        return share(vec, zbuf.at[n, h], nr, mr, zs, zr, n % 2, h, True)

    def share_c(vec, n, h):
        return share(vec, cbuf.at[n, h], nc, mc, cs, cr, n % 2, h, False)

    def back_part(k, h, dest):
        cols = block(dest * sv, sv)
        if k == 0:
            if h == 0:
                build_fa(dest)
                val = dot(y0[...], fa[:, cols])
                bacc[1, dest] = val[hz:]
                return val[:hz]
            return bacc[1, dest]
        val = bacc[h, dest]
        q = chip_at(1) * 2
        for i in range(2):
            val = val + dot(yb[k, h, q + i], fa[block((q + i) * sr, sr), cols])
        return val

    def back_grow(k, h, q, fresh):
        for d in range(nr):
            cols = slice(d * sv, (d + 1) * sv)
            val = dot(yb[k, h, q], fa[block(q * sr, sr), cols])
            val = val + dot(yb[k, h, q + 1], fa[block((q + 1) * sr, sr), cols])
            bacc[h, d] = val if fresh else bacc[h, d] + val

    def back_start(k, h):
        col_pack(bsend.at[k, h, 0], back_part(k, h, jnp.where(inner, cross, far)))
        slot = jnp.where(inner, 3, 0)
        send(bsend.at[k, h, 0], brecv.at[k, h, slot], bs, br, h, 0, slot, jnp.where(inner, cross, mate), mc)
        settle((id(bs), h, 1))
        relay[h] = back_part(k, h, jnp.where(inner, far, cross))

        @pl.when(outer)
        def _():
            col_pack(bsend.at[k, h, 1], relay[h])
            copy_to(bsend.at[k, h, 1], brecv.at[k, h, 1], bs.at[h, 1], br.at[h, 1], cross, mc).start()

        col_pack(bsend.at[k, h, 2], back_part(k, h, mate))
        send(bsend.at[k, h, 2], brecv.at[k, h, 2], bs, br, h, 2, 2, mate, mc)
        vox[k, h] = back_part(k, h, mr)

    def back_arrived(k, h, slot):
        copy_to(bsend.at[k, h, slot], brecv.at[k, h, slot], bs.at[h, slot], br.at[h, slot], mate, mc).wait_recv()
        return col_unpack(brecv.at[k, h, slot], hz)

    def back_relay(k, h):
        @pl.when(inner)
        def _():
            col_pack(bsend.at[k, h, 1], relay[h] + back_arrived(k, h, 0))
            copy_to(bsend.at[k, h, 1], brecv.at[k, h, 1], bs.at[h, 1], br.at[h, 1], far, mc).start()

        pending[id(bs), h, 1] = copy_to(bsend.at[k, h, 1], brecv.at[k, h, 1], bs.at[h, 1], br.at[h, 1], mate, mc)

    def back_sum(k, h):
        @pl.when(inner)
        def _():
            vox[k, h] = vox[k, h] + back_arrived(k, h, 3)

        total = vox[k, h] + back_arrived(k, h, 2)
        return total + back_arrived(k, h, 1)

    def fwd_grow(k, h, origin, fresh):
        for q in range(nch):
            cols = slice(2 * q * sr, 2 * (q + 1) * sr)
            val = dot(xb[h, origin], ba[block(origin * sv, sv), cols])
            for i in range(2):
                half = val[:, i * sr:(i + 1) * sr]
                fpart[k, h, 2 * q + i] = half if fresh else fpart[k, h, 2 * q + i] + half

    def vox_take(k, h, origin):
        val = col_unpack(vgat.at[k, h, origin], hz)
        vfull[h, origin] = val
        xb[h, origin] = val.astype(jnp.bfloat16)

    def passed(k, h, origin, n, row):
        own = vgat.at[k, h, origin]
        return copy_to(own, own, vs.at[h, n], vr.at[h, origin], row, mc)

    def vox_send(k, h):
        @pl.when(inner)
        def _():
            if k:
                passed(k, h, mr, 2, far).wait_send()
                passed(k, h, far, 3, mate).wait_send()
            passed(k, h, mr, 2, far).start()

        own = vgat.at[k, h, mr]
        send(own, own, vs, vr, h, 1, mr, cross, mc)
        send(own, own, vs, vr, h, 0, mr, mate, mc)

    def vox_early(k, h):
        @pl.when(inner)
        def _():
            passed(k, h, far, 3, mate).wait_recv()
            passed(k, h, far, 3, mate).start()

        @pl.when(outer)
        def _():
            passed(k, h, mate, 0, mate).wait_recv()

        vox_take(k, h, early)

    def fwd_send(k, h):
        local = []
        for s in range(nch - 1, -1, -1):
            q = chip_at(s) * 2
            val = dot(xb[h, late], ba[block(late * sv, sv), block(q * sr, 2 * sr)])
            for i in range(2):
                fpart[k, h, q + i] = fpart[k, h, q + i] + val[:, i * sr:(i + 1) * sr]
            local.append(send(fpart.at[k, h, q + 1 - core], drecv.at[k, h, s], ds_, dr, h, s, s, mr, partner))
        return local

    def fwd_pass(k, h, local):
        copies = []
        for s, other in zip(range(nch - 1, -1, -1), local):
            q = chip_at(s) * 2 + core
            other.wait_recv()
            part = fpart[k, h, q] + drecv[k, h, s]
            if s:
                col_pack(fsend.at[k, h, s], part)
                copies.append(send(fsend.at[k, h, s], frecv.at[k, h, s], fs, fr, h, s, s, mr, q))
            else:
                ray[k + 1, h] = part
        return copies

    def fwd_sum(k, h, copies):
        total = ray[k + 1, h]
        for i, copy in enumerate(copies):
            copy.wait_recv()
            total = total + col_unpack(frecv.at[k, h, nch - 1 - i], hz)
        return total

    def flip(first, last):
        @pl.loop(first, last)
        def _(d):
            for j in range(sv // LANE):
                cols = slice(j * LANE, (j + 1) * LANE)
                both = jnp.concatenate([vfull[0, d, :, cols], vfull[1, d, :, cols]], axis=0)
                vrow[block(d * sv + j * LANE, LANE), :] = both.T

    alphas = [[None, None] for _ in range(ITERS)]
    betas = [[None, None] for _ in range(ITERS + 1)]
    run = {}

    def update_dir(k):
        alpha = merge(*alphas[k])
        inv_alpha = 1.0 / alpha
        if k == 0:
            run["rho_bar"] = alpha
            sdir[...] = vrow[...] * inv_alpha
        else:
            theta = run["sine"] * alpha
            run["rho_bar"] = -run["cosine"] * alpha
            sdir[...] = vrow[...] * inv_alpha - (theta / run["rho"]) * sdir[...]

    def update_sol(k):
        beta = merge(*betas[k + 1])
        rho_bar = run["rho_bar"]
        rho = jnp.sqrt(rho_bar * rho_bar + beta * beta)
        run["rho"] = rho
        run["cosine"] = rho_bar / rho
        run["sine"] = beta / rho
        phi = run["cosine"] * run["phi_bar"]
        run["phi_bar"] = run["sine"] * run["phi_bar"]
        if k + 1 == ITERS:
            res[0:8] = jnp.broadcast_to(phi / rho, (8, z))
            res[8:16] = jnp.broadcast_to(run["phi_bar"], (8, z))
            return
        step = (phi / rho) * sdir[...]
        sol[...] = step if k == 0 else sol[...] + step

    def half(h):
        beta_of = None
        for k in range(ITERS):
            back_start(k, h)
            if k == 0 and h == 0:
                build_ba(mr)
                build_ba(early)
            yield
            back_relay(k, h)
            if k == 0 and h == 0:
                build_ba(cross)
                build_ba(late)
            yield
            total = back_sum(k, h)
            if k:
                betas[k][h] = root(beta_of)
            elif not h:
                run["phi_bar"] = root(first_norm)
                betas[0] = [run["phi_bar"], run["phi_bar"]]
            beta = betas[k][h]
            raw = total * wide(column(1.0 / beta, h), sv)
            if k:
                raw = raw - wide(column(beta / alphas[k - 1][h], h), sv) * vox[k - 1, h]
            vox[k, h] = raw
            col_pack(vgat.at[k, h, mr], raw)
            vox_send(k, h)
            alpha_of = share_z(row_squares(raw), 2 * k + 1, h)
            vox_take(k, h, mr)
            fwd_grow(k, h, mr, True)
            if k and h:
                update_sol(k - 1)
            yield
            vox_early(k, h)
            fwd_grow(k, h, early, False)
            yield
            passed(k, h, cross, 0, mate).wait_recv()
            vox_take(k, h, cross)
            fwd_grow(k, h, cross, False)
            yield
            passed(k, h, late, 0, mate).wait_recv()
            vox_take(k, h, late)
            local = fwd_send(k, h)
            alpha_of = share_c(alpha_of(), 2 * k + 1, h)
            yield
            copies = fwd_pass(k, h, local)
            if h:
                flip(0, nr)
            yield
            total = fwd_sum(k, h, copies)
            alpha = root(alpha_of)
            alphas[k][h] = alpha
            raw = total * wide(column(1.0 / alpha, h), sr)
            raw = raw - wide(column(alpha / beta, h), sr) * ray[k, h]
            n = 2 * k + 2
            if k + 1 == ITERS:
                beta_of = share_all(row_squares(raw), h)
                if h:
                    update_dir(k)
                yield
                betas[k + 1][h] = root(beta_of)
                return
            ray[k + 1, h] = raw
            own = yb.at[k + 1, h, mc]
            own[...] = raw.astype(jnp.bfloat16)
            across = [send(own, own, gs, gr, h, 0, 0, mr, partner)]
            for s in range(nch - 1, 0, -1):
                across.append(send(own, own, gs, gr, h, s, s, mr, chip_at(s) * 2 + core))
            beta_of = share_c(row_squares(raw), n, h)
            if h:
                update_dir(k)
            yield
            across[0].wait_recv()
            back_grow(k + 1, h, chip * 2, True)
            yield
            hand = []
            for s in range(nch - 1, 0, -1):
                across[nch - s].wait_recv()
                origin = chip_at(s) * 2 + core
                given = yb.at[k + 1, h, origin]
                hand.append(send(given, given, hs, hr, h, s, s, mr, partner))
            beta_of = share_z(beta_of(), n, h)
            yield
            for s in range(nch - 1, 0, -1):
                hand[nch - 1 - s].wait_recv()
                if s > 1:
                    back_grow(k + 1, h, chip_at(s) * 2, False)

    def build_fa(dest):
        wide_by = sv // tile

        @pl.loop(0, tr)
        def _(i):
            for j in range(wide_by):
                fa[block(i * tile, tile), block(dest * sv + j * tile, tile)] = pick(i, dest * wide_by + j)

    def build_ba(origin):
        wide_by = sv // tile

        @pl.loop(0, wide_by)
        def _(j):
            for i in range(tr):
                ba[block(origin * sv + j * tile, tile), i * tile:(i + 1) * tile] = pick(i, origin * wide_by + j).T

    place = jnp.broadcast_to(place_of[...], (LANE, slots)).T
    slot_of = lax.broadcasted_iota(jnp.int32, (slots, LANE), 0)
    for i in range(inv.shape[0]):
        spot = lax.broadcasted_iota(jnp.int32, (slots, LANE), 1) + i * LANE
        inv_row[i:i + 1, :] = jnp.min(jnp.where(place == spot, slot_of, slots), axis=0, keepdims=True)
    move = pltpu.make_async_copy(inv_row, inv, io.at[1])
    move.start()
    tiles[slots] = jnp.zeros((tile, tile), tiles.dtype)
    load_sino.wait()
    total = squares(sino[...])
    for i in range(tr):
        y0[:, i * tile:(i + 1) * tile] = sino[i * tile:(i + 1) * tile, :].T.astype(jnp.bfloat16)
    own = sino[block(mc * sr, sr), :].T
    ray[0, 0] = own[:hz]
    ray[0, 1] = own[hz:]
    move.wait()
    for load in load_tiles:
        load.wait()

    pl.semaphore_wait(barrier, nr * nc - 1)
    first_norm = share_z(total, 0, 0)
    halves = [half(0), half(1)]
    for h in ORDER:
        next(halves[h], None)
    update_sol(ITERS - 1)
    for key in list(pending):
        settle(key)

    @pl.when(inner)
    def _():
        for h in range(2):
            passed(0, h, mr, 2, far).wait_send()
            passed(0, h, far, 3, mate).wait_send()


def finish_kernel(x, d, scale, out, last, val, sems):
    parts = sems.shape[0]
    n = x.shape[0] // parts
    last[...] = scale[8:9, :]
    stores = []
    for i in range(parts):
        rows = pl.ds(i * n, n)
        val[rows, :] = x[rows, :] + scale[0:1, :] * d[rows, :]
        stores.append(pltpu.make_async_copy(val.at[rows], out.at[rows], sems.at[i]))
        stores[i].start()
    for store in stores:
        store.wait()


def body(nr, nc, tile_values, tile_rows, tile_cols, tile_count, sinogram):
    values = tile_values[0, 0]
    slots, tile = values.shape[0], values.shape[1]
    mb, z = sinogram.shape
    nb = TC * tile
    tr = mb // tile
    sv, sr = nb // nr, mb // nc
    if nr != 4 or nc != 8 or sr % LANE or sv % LANE or z != LANE:
        return body_rows(nr, nc, tile_values, tile_rows, tile_cols, tile_count, sinogram)
    ids = jnp.arange(slots, dtype=jnp.int32)[None, :]
    place = jnp.where(ids < tile_count, tile_rows[0] * TC + tile_cols[0], -1)
    nch, hz = nc // 2, z // 2
    f32, bf16, i16 = jnp.float32, jnp.bfloat16, jnp.int16
    dma, vmem_of = pltpu.SemaphoreType.DMA, pltpu.VMEM
    vmem = pl.BlockSpec(memory_space=pltpu.VMEM)
    hbm = pl.BlockSpec(memory_space=pltpu.HBM)
    pb, pf = sv // LANE * hz + PAD, sr // LANE * hz + PAD
    norms = 2 * ITERS + 1
    spots = tr * TC // LANE
    scratch = [
        vmem_of((slots + 1, tile, tile), bf16), vmem_of((mb, z), f32),
        vmem_of((spots, LANE), jnp.int32), pltpu.SMEM((spots, LANE), jnp.int32),
        vmem_of((mb, nb), bf16), vmem_of((nb, mb), bf16), vmem_of((z, mb), bf16),
        vmem_of((ITERS, 2, nc, hz, sr), bf16), vmem_of((2, nr, hz, sv), f32),
        vmem_of((ITERS, 2, nc, hz, sr), f32), vmem_of((ITERS, 2, nch, hz, sr), f32),
        vmem_of((2, nr, hz, sv), bf16), vmem_of((2, nr, hz, sv), f32),
        vmem_of((ITERS + 1, 2, hz, sr), f32), vmem_of((ITERS, 2, hz, sv), f32), vmem_of((2, hz, sv), f32),
        vmem_of((nb, z), f32),
        vmem_of((ITERS, 2, nr, pb, LANE), i16), vmem_of((ITERS, 2, nr, pb, LANE), i16),
        vmem_of((ITERS, 2, nr, pb, LANE), i16),
        vmem_of((ITERS, 2, nch, pf, LANE), i16), vmem_of((ITERS, 2, nch, pf, LANE), i16),
        vmem_of((norms, 2, nr, 8, z), f32), vmem_of((norms, 2, nc, 8, z), f32),
        vmem_of((2, nr * nc, 1, z), f32),
    ] + [dma((2, nr))] * 4 + [dma((2, nch))] * 8 + [dma((2, 2))] * 4 + [dma((2,))] * 2 + [dma((6,))]
    part = jax.ShapeDtypeStruct((nb, z), f32)
    sol, step, scale = pl.pallas_call(
        functools.partial(kernel, nr, nc),
        out_shape=(part, part, jax.ShapeDtypeStruct((16, z), f32)),
        in_specs=[vmem, hbm, hbm],
        out_specs=(vmem, vmem, vmem),
        scratch_shapes=scratch,
        compiler_params=pltpu.CompilerParams(
            collective_id=0, has_side_effects=True, vmem_limit_bytes=GRANT),
    )(place, values, sinogram)
    sol, last = pl.pallas_call(
        finish_kernel,
        out_shape=(part, jax.ShapeDtypeStruct((1, z), f32)),
        in_specs=[vmem, vmem, vmem],
        out_specs=(hbm, vmem),
        scratch_shapes=[vmem_of((nb, z), f32), dma((4,))],
        compiler_params=pltpu.CompilerParams(vmem_limit_bytes=8 * 1024 * 1024),
    )(sol, step, scale)
    return sol, last[0]


def solution(mesh):
    nr, nc = mesh.shape["row"], mesh.shape["col"]
    in_specs = (
        P("row", "col", None, None, None),
        P("row", "col", None),
        P("row", "col", None),
        P("row", "col"),
        P("row", None),
    )
    return jax.shard_map(
        functools.partial(body, nr, nc), mesh=mesh, in_specs=in_specs,
        out_specs=(P("col", None), P()), check_vma=False)
```

```python
import functools

import jax
import jax.numpy as jnp
from jax import lax
from jax.experimental import pallas as pl
from jax.experimental.pallas import tpu as pltpu
from jax.sharding import PartitionSpec as P

TC = 16
ITERS = 3
EPSILON = 1e-06
PAD = 16
TOP = 32000.0
FINE = 64.0
LANE = 128
GRANT = 53000 * 1024
ORDER = [int(one) for one in '0001001001001011010110110010010010110101101100100101111101']
MESH = pl.DeviceIdType.MESH


def pack(val):
    top = jnp.max(jnp.abs(val), axis=0, keepdims=True)
    exponent = jnp.ceil(jnp.log2(jnp.maximum(top, 1e-30)))
    scale = TOP * jnp.exp2(-exponent)
    coded = jnp.round(jnp.clip(val * scale, -32767.0, 32767.0))
    coded = coded.astype(jnp.int32).astype(jnp.int16)
    rows = jnp.broadcast_to(exponent, (PAD, val.shape[1]))
    return coded, rows.astype(jnp.int32).astype(jnp.int16)


def store_packet(ref, val):
    n = val.shape[0]
    coded, rows = pack(val)
    ref[pl.ds(0, n), :] = coded
    ref[pl.ds(n, PAD), :] = rows


def load_packet(ref):
    n = ref.shape[0] - PAD
    exponent = ref[pl.ds(n, PAD), :].astype(jnp.int32).astype(jnp.float32)[:1]
    scale = jnp.exp2(exponent) * (1.0 / TOP)
    return ref[pl.ds(0, n), :].astype(jnp.int32).astype(jnp.float32) * scale


def dot(a, b):
    return jnp.dot(a, b, preferred_element_type=jnp.float32)


def root(total_of):
    return jnp.sqrt(total_of() + EPSILON)


def squares(vec):
    return jnp.sum(vec * vec, axis=0, keepdims=True)


def kernel_rows(
    nr, nc, inv, tiles, sino, sol, res,
    facc, bacc, sq, fa, ba, ybf, xbf, ray, vox, vfull, sdir,
    bsend, brecv, vgat, dsend, drecv, fsend, frecv, rgat, nrow, ncol, nlast,
    bs, br, vs, vr, ds_, dr, fs, fr, gs, gr, hs, hr, rs, rr, cs, cr, ls, lr,
):
    mr = lax.axis_index("row")
    mc = lax.axis_index("col")
    nch = nc // 2
    chip = mc // 2
    core = mc % 2
    partner = chip * 2 + (1 - core)
    tile = tiles.shape[1]
    mb, z = sino.shape
    nb = sol.shape[0]
    tr, tc = mb // tile, nb // tile
    sv, sr = nb // nr, mb // nc

    barrier = pltpu.get_barrier_semaphore()
    for s in range(1, nr):
        pl.semaphore_signal(barrier, 1, device_id=(lax.rem(mr + s, nr), mc), device_id_type=MESH)
    for s in range(1, nc):
        pl.semaphore_signal(barrier, 1, device_id=(mr, lax.rem(mc + s, nc)), device_id_type=MESH)

    def send(src, dst, ssem, rsem, row, col):
        copy = pltpu.make_async_remote_copy(
            src_ref=src, dst_ref=dst, send_sem=ssem, recv_sem=rsem,
            device_id=(row, col), device_id_type=MESH)
        copy.start()
        sent.append(copy)
        return copy

    sent = []

    def pick(i, j):
        slot = inv[i * tc + j]
        block = tiles[jnp.maximum(slot, 0)]
        return jnp.where(slot >= 0, block, jnp.zeros_like(block))

    @pl.loop(0, tc)
    def _(j):
        first = pl.multiple_of(j * tile, tile)
        for i in range(tr):
            ba[pl.ds(first, tile), i * tile:(i + 1) * tile] = pick(i, j).T

    def share(vec, buf, n, me, ssem, rsem, over_row):
        buf[me] = jnp.broadcast_to(vec, (8, z))
        copies = []
        for s in range(1, n):
            peer = lax.rem(me + s, n)
            place = (peer, mc) if over_row else (mr, peer)
            copies.append(send(buf.at[me], buf.at[me], ssem.at[s], rsem.at[s], *place))

        def finish():
            for copy in copies:
                copy.wait_recv()
            total = buf[0]
            for q in range(1, n):
                total = total + buf[q]
            return total[:1]

        return finish

    line = nr == 4
    inner = (mr == 1) | (mr == 2)
    left = mr < 2
    mate = mr + 1 - 2 * lax.rem(mr, 2)
    cross = jnp.where(left, 2, 1)
    far = jnp.where(left, 3, 0)
    early = jnp.where(inner, far, mate)
    late = jnp.where(inner, mate, far)
    inner_sent = []

    def row_copy(src, dst, ssem, rsem, row):
        return pltpu.make_async_remote_copy(
            src_ref=src, dst_ref=dst, send_sem=ssem, recv_sem=rsem,
            device_id=(row, mc), device_id_type=MESH)

    def back_part(k, dest):
        rows = pl.ds(pl.multiple_of(dest * sv, sv), sv)
        if k == 0:
            return dot(ba[rows, :], ybf[...])
        late = lax.rem(chip + 1, nch) * 2 * sr
        cols = pl.ds(pl.multiple_of(late, 2 * sr), 2 * sr)
        return bacc[rows, :] + dot(ba[rows, cols], ybf[cols, :])

    def back_arrived(k, slot):
        row_copy(bsend.at[k, slot], brecv.at[k, slot], bs.at[k, slot], br.at[k, slot], mate).wait_recv()

    def back_start(k):
        if line:
            store_packet(bsend.at[k, 0], back_part(k, jnp.where(inner, cross, far)))
            slot = jnp.where(inner, 3, 0)
            send(bsend.at[k, 0], brecv.at[k, slot], bs.at[k, 0], br.at[k, slot],
                 jnp.where(inner, cross, mate), mc)
            part = back_part(k, jnp.where(inner, far, cross))

            @pl.when(jnp.logical_not(inner))
            def _():
                store_packet(bsend.at[k, 1], part)

            @pl.when(inner)
            def _():
                back_arrived(k, 0)
                store_packet(bsend.at[k, 1], part + load_packet(brecv.at[k, 0]))

            send(bsend.at[k, 1], brecv.at[k, 1], bs.at[k, 1], br.at[k, 1], jnp.where(inner, far, cross), mc)
            store_packet(bsend.at[k, 2], back_part(k, mate))
            send(bsend.at[k, 2], brecv.at[k, 2], bs.at[k, 2], br.at[k, 2], mate, mc)
            vox[k] = back_part(k, mr)
            return None
        copies = []
        for s in list(range(1, nr)) + [0]:
            dest = lax.rem(mr + s, nr)
            part = back_part(k, dest)
            if s:
                store_packet(bsend.at[k, s], part)
                copies.append(send(bsend.at[k, s], brecv.at[k, s], bs.at[k, s], br.at[k, s], dest, mc))
            else:
                vox[k] = part
        return copies

    def back_sum(k, copies):
        if line:
            @pl.when(inner)
            def _():
                back_arrived(k, 3)
                vox[k] = vox[k] + load_packet(brecv.at[k, 3])

            total = vox[k]
            for slot in (2, 1):
                back_arrived(k, slot)
                total = total + load_packet(brecv.at[k, slot])
            return total
        total = vox[k]
        for i, copy in enumerate(copies):
            copy.wait_recv()
            total = total + load_packet(brecv.at[k, i + 1])
        return total

    def vox_take(k, origin):
        val = load_packet(vgat.at[k, origin])
        rows = pl.ds(pl.multiple_of(origin * sv, sv), sv)
        vfull[rows, :] = val
        xbf[rows, :] = val.astype(jnp.bfloat16)

    def grow(acc, mat, vec, first, depth, fresh):
        cols = pl.ds(pl.multiple_of(first, depth), depth)

        @pl.loop(0, acc.shape[0] // sv)
        def _(i):
            rows = pl.ds(pl.multiple_of(i * sv, sv), sv)
            val = dot(mat[rows, cols], vec[cols, :])
            acc[rows, :] = val if fresh else acc[rows, :] + val

    def vox_gather(k):
        store_packet(vgat.at[k, mr], vox[k])
        if line:
            def passed(origin, n, row):
                return row_copy(vgat.at[k, origin], vgat.at[k, origin], vs.at[k, n], vr.at[k, origin], row)

            @pl.when(inner)
            def _():
                passed(mr, 2, far).start()

            send(vgat.at[k, mr], vgat.at[k, mr], vs.at[k, 1], vr.at[k, mr], cross, mc)
            send(vgat.at[k, mr], vgat.at[k, mr], vs.at[k, 0], vr.at[k, mr], mate, mc)
            inner_sent.append(passed(mr, 2, far))
            inner_sent.append(passed(far, 3, mate))
            vox_take(k, mr)
            grow(facc, fa, xbf, mr * sv, sv, True)

            @pl.when(inner)
            def _():
                passed(far, 3, mate).wait_recv()
                passed(far, 3, mate).start()

            @pl.when(jnp.logical_not(inner))
            def _():
                passed(mate, 0, mate).wait_recv()

            vox_take(k, early)
            grow(facc, fa, xbf, early * sv, sv, False)
            passed(cross, 0, mate).wait_recv()
            vox_take(k, cross)
            grow(facc, fa, xbf, cross * sv, sv, False)
            passed(late, 0, mate).wait_recv()
            vox_take(k, late)
        else:
            copies = [
                send(vgat.at[k, mr], vgat.at[k, mr], vs.at[k, s], vr.at[k, s], lax.rem(mr + s, nr), mc)
                for s in range(1, nr)
            ]
            for copy in copies:
                copy.wait_recv()
            for q in range(nr):
                vox_take(k, q)
        return share(squares(vfull[...]), ncol.at[k], nc, mc, cs.at[k], cr.at[k], False)

    def fwd_part(first):
        rows = pl.ds(first, sr)
        if line:
            cols = pl.ds(pl.multiple_of(late * sv, sv), sv)
            return facc[rows, :] + dot(fa[rows, cols], xbf[cols, :])
        return dot(fa[rows, :], xbf[...])

    def fwd_start(k):
        order = list(range(1, nch)) + [0]
        local = []
        for s in order:
            q = lax.rem(chip + s, nch)
            first = pl.multiple_of((q * 2 + 1 - core) * sr, sr)
            dsend[k, s] = fwd_part(first)
            local.append(send(dsend.at[k, s], drecv.at[k, s], ds_.at[k, s], dr.at[k, s], mr, partner))
        copies = []
        for s, other in zip(order, local):
            q = lax.rem(chip + s, nch)
            first = pl.multiple_of((q * 2 + core) * sr, sr)
            part = fwd_part(first)
            other.wait_recv()
            part = part + drecv[k, s]
            if s:
                store_packet(fsend.at[k, s], part)
                copies.append(send(fsend.at[k, s], frecv.at[k, s], fs.at[k, s], fr.at[k, s], mr, q * 2 + core))
            else:
                ray[k + 1] = part
        return copies

    def fwd_sum(k, copies):
        total = ray[k + 1]
        for i, copy in enumerate(copies):
            copy.wait_recv()
            total = total + load_packet(frecv.at[k, i + 1])
        return total

    def ray_gather(k):
        store_packet(rgat.at[k, mc], ray[k + 1])
        across = [send(rgat.at[k, mc], rgat.at[k, mc], gs.at[k, 0], gr.at[k, 0], mr, partner)]
        for s in range(1, nch):
            peer = lax.rem(chip + s, nch) * 2 + core
            across.append(send(rgat.at[k, mc], rgat.at[k, mc], gs.at[k, s], gr.at[k, s], mr, peer))
        hand = [None]

        def take(origin):
            val = load_packet(rgat.at[k, origin])
            sq[origin] = jnp.broadcast_to(squares(val), (8, z))
            ybf[pl.ds(pl.multiple_of(origin * sr, sr), sr), :] = val.astype(jnp.bfloat16)

        take(mc)
        across[0].wait_recv()
        take(partner)
        grow(bacc, ba, ybf, chip * 2 * sr, 2 * sr, True)
        for s in range(1, nch):
            across[s].wait_recv()
            origin = lax.rem(chip + nch - s, nch) * 2 + core
            hand.append(send(rgat.at[k, origin], rgat.at[k, origin], hs.at[k, s], hr.at[k, s], mr, partner))
            take(origin)
        for s in range(1, nch):
            hand[s].wait_recv()
            origin = lax.rem(chip + nch - s, nch) * 2
            take(origin + 1 - core)
            if s + 1 < nch:
                grow(bacc, ba, ybf, origin * sr, 2 * sr, False)
        total = jnp.zeros((1, z), jnp.float32)
        for q in range(nc):
            total = total + sq[q][:1]
        return share(total, nrow.at[k + 1], nr, mr, rs.at[k + 1], rr.at[k + 1], True)

    ybf[...] = sino[...].astype(jnp.bfloat16)
    total = squares(sino[...])
    pl.semaphore_wait(barrier, nr - 1 + nc - 1)
    beta_of = share(total, nrow.at[0], nr, mr, rs.at[0], rr.at[0], True)
    copies = back_start(0)

    @pl.loop(0, tr)
    def _(i):
        first = pl.multiple_of(i * tile, tile)
        for j in range(tc):
            fa[pl.ds(first, tile), j * tile:(j + 1) * tile] = pick(i, j)

    beta = root(beta_of)
    ray[0] = sino[pl.ds(pl.multiple_of(mc * sr, sr), sr), :] * (1.0 / beta)
    vox[0] = back_sum(0, copies) * (1.0 / beta)
    alpha_of = vox_gather(0)
    phi_bar = beta
    for k in range(ITERS):
        copies = fwd_start(k)
        alpha = root(alpha_of)
        inv_alpha = 1.0 / alpha
        if k == 0:
            rho_bar = alpha
            sdir[...] = vfull[...] * inv_alpha
        else:
            theta = sine * alpha
            rho_bar = -cosine * alpha
            sdir[...] = vfull[...] * inv_alpha - (theta / rho) * sdir[...]
        vox[k] = vox[k] * inv_alpha
        ray_raw = fwd_sum(k, copies) * inv_alpha - alpha * ray[k]
        last = k + 1 == ITERS
        if last:
            total = share(squares(ray_raw), nlast, nc, mc, ls, lr, False)()
            beta = root(share(total, nrow.at[k + 1], nr, mr, rs.at[k + 1], rr.at[k + 1], True))
        else:
            ray[k + 1] = ray_raw
            beta_of = ray_gather(k)
            copies = back_start(k + 1)
            beta = root(beta_of)
            ray[k + 1] = ray[k + 1] * (1.0 / beta)
        rho = jnp.sqrt(rho_bar * rho_bar + beta * beta)
        cosine = rho_bar / rho
        sine = beta / rho
        phi = cosine * phi_bar
        phi_bar = sine * phi_bar
        step = (phi / rho) * sdir[...]
        sol[...] = step if k == 0 else sol[...] + step
        if not last:
            vox[k + 1] = back_sum(k + 1, copies) * (1.0 / beta) - beta * vox[k]
            alpha_of = vox_gather(k + 1)
    res[...] = jnp.broadcast_to(phi_bar, res.shape)
    for copy in sent:
        copy.wait_send()
    if line:
        @pl.when(inner)
        def _():
            for copy in inner_sent:
                copy.wait_send()


def body_rows(nr, nc, tile_values, tile_rows, tile_cols, tile_count, sinogram):
    values = tile_values[0, 0]
    slots, tile = values.shape[0], values.shape[1]
    mb, z = sinogram.shape
    nb = TC * tile
    tr = mb // tile
    place = tile_rows[0, 0] * TC + tile_cols[0, 0]
    ids = jnp.arange(slots, dtype=jnp.int32)
    place = jnp.where(ids < tile_count[0, 0], place, -1)
    hit = place[None, :] == jnp.arange(tr * TC, dtype=jnp.int32)[:, None]
    inv = jnp.sum(jnp.where(hit, ids[None, :] + 1, 0), axis=1, dtype=jnp.int32) - 1
    nch = nc // 2
    sv, sr = nb // nr, mb // nc
    f32, bf16, i16 = jnp.float32, jnp.bfloat16, jnp.int16
    dma = pltpu.SemaphoreType.DMA
    vmem = pl.BlockSpec(memory_space=pltpu.VMEM)
    scratch = [
        pltpu.VMEM((mb, z), f32), pltpu.VMEM((nb, z), f32), pltpu.VMEM((nc, 8, z), f32),
        pltpu.VMEM((mb, nb), bf16), pltpu.VMEM((nb, mb), bf16),
        pltpu.VMEM((mb, z), bf16), pltpu.VMEM((nb, z), bf16),
        pltpu.VMEM((ITERS + 1, sr, z), f32), pltpu.VMEM((ITERS, sv, z), f32),
        pltpu.VMEM((nb, z), f32), pltpu.VMEM((nb, z), f32),
        pltpu.VMEM((ITERS, nr, sv + PAD, z), i16), pltpu.VMEM((ITERS, nr, sv + PAD, z), i16),
        pltpu.VMEM((ITERS, nr, sv + PAD, z), i16),
        pltpu.VMEM((ITERS, nch, sr, z), f32), pltpu.VMEM((ITERS, nch, sr, z), f32),
        pltpu.VMEM((ITERS, nch, sr + PAD, z), i16), pltpu.VMEM((ITERS, nch, sr + PAD, z), i16),
        pltpu.VMEM((ITERS, nc, sr + PAD, z), i16),
        pltpu.VMEM((ITERS + 1, nr, 8, z), f32), pltpu.VMEM((ITERS, nc, 8, z), f32),
        pltpu.VMEM((nc, 8, z), f32),
        dma((ITERS, nr)), dma((ITERS, nr)), dma((ITERS, nr)), dma((ITERS, nr)),
        dma((ITERS, nch)), dma((ITERS, nch)), dma((ITERS, nch)), dma((ITERS, nch)),
        dma((ITERS, nch)), dma((ITERS, nch)), dma((ITERS, nch)), dma((ITERS, nch)),
        dma((ITERS + 1, nr)), dma((ITERS + 1, nr)), dma((ITERS, nc)), dma((ITERS, nc)),
        dma((nc,)), dma((nc,)),
    ]
    sol, res = pl.pallas_call(
        functools.partial(kernel_rows, nr, nc),
        out_shape=(jax.ShapeDtypeStruct((nb, z), f32), jax.ShapeDtypeStruct((8, z), f32)),
        in_specs=[pl.BlockSpec(memory_space=pltpu.SMEM), vmem, vmem],
        out_specs=(vmem, vmem),
        scratch_shapes=scratch,
        compiler_params=pltpu.CompilerParams(
            collective_id=0, has_side_effects=True, vmem_limit_bytes=60 * 1024 * 1024),
    )(inv, values, sinogram)
    return sol, res[0]


def col_pack(ref, val):
    h, n = val.shape
    groups = h // PAD
    mag = jnp.abs(val)
    top = mag[:PAD]
    for g in range(1, groups):
        top = jnp.maximum(top, mag[g * PAD:(g + 1) * PAD])
    top = jnp.max(top, axis=1, keepdims=True)
    exponent = jnp.ceil(jnp.log2(jnp.maximum(top, 1e-30)) * FINE)
    scale = jnp.concatenate([TOP * jnp.exp2(exponent * (-1.0 / FINE))] * groups, axis=0)
    coded = jnp.round(val * scale).astype(jnp.int32).astype(jnp.int16)
    for j in range(n // LANE):
        ref[pl.ds(j * h, h), :] = coded[:, j * LANE:(j + 1) * LANE]
    ref[pl.ds(n // LANE * h, PAD), :] = jnp.broadcast_to(exponent, (PAD, LANE)).astype(jnp.int32).astype(jnp.int16)


def col_unpack(ref, h):
    blocks = (ref.shape[0] - PAD) // h
    exponent = ref[pl.ds(blocks * h, PAD), :].astype(jnp.int32).astype(jnp.float32)
    scale = jnp.concatenate([jnp.exp2(exponent * (1.0 / FINE)) * (1.0 / TOP)] * (h // PAD), axis=0)
    return jnp.concatenate(
        [ref[pl.ds(j * h, h), :].astype(jnp.int32).astype(jnp.float32) * scale for j in range(blocks)], axis=1)


def row_squares(val):
    h, n = val.shape
    acc = jnp.zeros((h, LANE), jnp.float32)
    for j in range(n // LANE):
        part = val[:, j * LANE:(j + 1) * LANE]
        acc = acc + part * part
    acc = jnp.concatenate([acc] * (LANE // h), axis=0)
    return jnp.sum(acc.T, axis=0, keepdims=True)


def kernel(
    nr, nc, place_of, tiles_in, sino_in, sol, sdir, res,
    tiles, sino, inv_row, inv,
    fa, ba, y0, yb, bacc, fpart, drecv, xb, vfull, ray, vox, relay, vrow,
    bsend, brecv, vgat, fsend, frecv, zbuf, cbuf, abuf,
    bs, br, vs, vr, ds_, dr, fs, fr, gs, gr, hs, hr, zs, zr, cs, cr, as_, ar, io,
):
    mr = lax.axis_index("row")
    mc = lax.axis_index("col")
    nch = nc // 2
    chip = mc // 2
    core = mc % 2
    partner = chip * 2 + (1 - core)
    slots, tile = tiles_in.shape[0], tiles_in.shape[1]
    mb, z = sino.shape
    nb = sol.shape[0]
    tr, tc = mb // tile, nb // tile
    sv, sr = nb // nr, mb // nc
    hz = z // 2

    inner = (mr == 1) | (mr == 2)
    outer = jnp.logical_not(inner)
    left = mr < 2
    mate = mr + 1 - 2 * lax.rem(mr, 2)
    cross = jnp.where(left, 2, 1)
    far = jnp.where(left, 3, 0)
    early = jnp.where(inner, far, mate)
    late = jnp.where(inner, mate, far)

    barrier = pltpu.get_barrier_semaphore()
    for r in range(nr):
        for c in range(nc):
            if r or c:
                pl.semaphore_signal(
                    barrier, 1, device_id=(lax.rem(mr + r, nr), lax.rem(mc + c, nc)), device_id_type=MESH)
    load_sino = pltpu.make_async_copy(sino_in, sino, io.at[0])
    load_sino.start()
    load_tiles = []
    for i in range(4):
        some = pl.ds(slots // 4 * i, slots // 4)
        load_tiles.append(pltpu.make_async_copy(tiles_in.at[some], tiles.at[some], io.at[i + 2]))
        load_tiles[i].start()

    pending = {}

    def copy_to(src, dst, ssem, rsem, row, col):
        return pltpu.make_async_remote_copy(
            src_ref=src, dst_ref=dst, send_sem=ssem, recv_sem=rsem,
            device_id=(row, col), device_id_type=MESH)

    def settle(key):
        if key in pending:
            pending.pop(key).wait_send()

    def send(src, dst, ssems, rsems, h, s, slot, row, col):
        key = (id(ssems), h, s)
        settle(key)
        copy = copy_to(src, dst, ssems.at[h, s], rsems.at[h, slot], row, col)
        copy.start()
        pending[key] = copy
        return copy

    def chip_at(s):
        return (chip // 2 + s // 2) % 2 * 2 + (chip % 2 + s % 2) % 2

    def block(first, size):
        return pl.ds(pl.multiple_of(first, size), size)

    def pick(i, j):
        per = LANE // tc
        return tiles[inv[i // per, i % per * tc + j]]

    def column(row, h):
        return jnp.broadcast_to(row, (z, z)).T[h * hz:(h + 1) * hz]

    def wide(col, n):
        return jnp.concatenate([col] * (n // LANE), axis=1)

    def merge(a, b):
        lane = lax.broadcasted_iota(jnp.int32, (1, z), 1)
        return jnp.where(lane < hz, a, b)

    def share(vec, buf, n, me, ssems, rsems, kind, h, over_row):
        key = (id(ssems), kind, h)
        settle(key)
        buf[me] = jnp.broadcast_to(vec, (8, z))
        for s in range(1, n):
            peer = lax.rem(me + s, n)
            place = (peer, mc) if over_row else (mr, peer)
            copy_to(buf.at[me], buf.at[me], ssems.at[kind, h], rsems.at[kind, h], *place).start()
        others = buf.at[pl.ds(0, n - 1)]
        place = (lax.rem(mr + 1, nr), mc)
        pending[key] = copy_to(others, others, ssems.at[kind, h], rsems.at[kind, h], *place)

        def finish():
            copy_to(others, others, ssems.at[kind, h], rsems.at[kind, h], *place).wait_recv()
            total = buf[0]
            for q in range(1, n):
                total = total + buf[q]
            return total[:1]

        return finish

    def share_all(vec, h):
        buf, me = abuf.at[h], mr * nc + mc
        buf[me] = vec
        for r in range(nr):
            for c in range(nc):
                if r or c:
                    copy_to(buf.at[me], buf.at[me], as_.at[h], ar.at[h],
                            lax.rem(mr + r, nr), lax.rem(mc + c, nc)).start()
        others = buf.at[pl.ds(0, nr * nc - 1)]
        arrived = copy_to(others, others, as_.at[h], ar.at[h], lax.rem(mr + 1, nr), mc)
        pending[id(as_), h] = arrived

        def finish():
            arrived.wait_recv()
            total = buf[0]
            for q in range(1, nr * nc):
                total = total + buf[q]
            return total

        return finish

    def share_z(vec, n, h):
        return share(vec, zbuf.at[n, h], nr, mr, zs, zr, n % 2, h, True)

    def share_c(vec, n, h):
        return share(vec, cbuf.at[n, h], nc, mc, cs, cr, n % 2, h, False)

    def back_part(k, h, dest):
        cols = block(dest * sv, sv)
        if k == 0:
            if h == 0:
                build_fa(dest)
                val = dot(y0[...], fa[:, cols])
                bacc[1, dest] = val[hz:]
                return val[:hz]
            return bacc[1, dest]
        val = bacc[h, dest]
        q = chip_at(1) * 2
        for i in range(2):
            val = val + dot(yb[k, h, q + i], fa[block((q + i) * sr, sr), cols])
        return val

    def back_grow(k, h, q, fresh):
        for d in range(nr):
            cols = slice(d * sv, (d + 1) * sv)
            val = dot(yb[k, h, q], fa[block(q * sr, sr), cols])
            val = val + dot(yb[k, h, q + 1], fa[block((q + 1) * sr, sr), cols])
            bacc[h, d] = val if fresh else bacc[h, d] + val

    def back_start(k, h):
        col_pack(bsend.at[k, h, 0], back_part(k, h, jnp.where(inner, cross, far)))
        slot = jnp.where(inner, 3, 0)
        send(bsend.at[k, h, 0], brecv.at[k, h, slot], bs, br, h, 0, slot, jnp.where(inner, cross, mate), mc)
        settle((id(bs), h, 1))
        relay[h] = back_part(k, h, jnp.where(inner, far, cross))

        @pl.when(outer)
        def _():
            col_pack(bsend.at[k, h, 1], relay[h])
            copy_to(bsend.at[k, h, 1], brecv.at[k, h, 1], bs.at[h, 1], br.at[h, 1], cross, mc).start()

        col_pack(bsend.at[k, h, 2], back_part(k, h, mate))
        send(bsend.at[k, h, 2], brecv.at[k, h, 2], bs, br, h, 2, 2, mate, mc)
        vox[k, h] = back_part(k, h, mr)

    def back_arrived(k, h, slot):
        copy_to(bsend.at[k, h, slot], brecv.at[k, h, slot], bs.at[h, slot], br.at[h, slot], mate, mc).wait_recv()
        return col_unpack(brecv.at[k, h, slot], hz)

    def back_relay(k, h):
        @pl.when(inner)
        def _():
            col_pack(bsend.at[k, h, 1], relay[h] + back_arrived(k, h, 0))
            copy_to(bsend.at[k, h, 1], brecv.at[k, h, 1], bs.at[h, 1], br.at[h, 1], far, mc).start()

        pending[id(bs), h, 1] = copy_to(bsend.at[k, h, 1], brecv.at[k, h, 1], bs.at[h, 1], br.at[h, 1], mate, mc)

    def back_sum(k, h):
        @pl.when(inner)
        def _():
            vox[k, h] = vox[k, h] + back_arrived(k, h, 3)

        total = vox[k, h] + back_arrived(k, h, 2)
        return total + back_arrived(k, h, 1)

    def fwd_grow(k, h, origin, fresh):
        for q in range(nch):
            cols = slice(2 * q * sr, 2 * (q + 1) * sr)
            val = dot(xb[h, origin], ba[block(origin * sv, sv), cols])
            for i in range(2):
                half = val[:, i * sr:(i + 1) * sr]
                fpart[k, h, 2 * q + i] = half if fresh else fpart[k, h, 2 * q + i] + half

    def vox_take(k, h, origin):
        val = col_unpack(vgat.at[k, h, origin], hz)
        vfull[h, origin] = val
        xb[h, origin] = val.astype(jnp.bfloat16)

    def passed(k, h, origin, n, row):
        own = vgat.at[k, h, origin]
        return copy_to(own, own, vs.at[h, n], vr.at[h, origin], row, mc)

    def vox_send(k, h):
        @pl.when(inner)
        def _():
            if k:
                passed(k, h, mr, 2, far).wait_send()
                passed(k, h, far, 3, mate).wait_send()
            passed(k, h, mr, 2, far).start()

        own = vgat.at[k, h, mr]
        send(own, own, vs, vr, h, 1, mr, cross, mc)
        send(own, own, vs, vr, h, 0, mr, mate, mc)

    def vox_early(k, h):
        @pl.when(inner)
        def _():
            passed(k, h, far, 3, mate).wait_recv()
            passed(k, h, far, 3, mate).start()

        @pl.when(outer)
        def _():
            passed(k, h, mate, 0, mate).wait_recv()

        vox_take(k, h, early)

    def fwd_send(k, h):
        local = []
        for s in range(nch - 1, -1, -1):
            q = chip_at(s) * 2
            val = dot(xb[h, late], ba[block(late * sv, sv), block(q * sr, 2 * sr)])
            for i in range(2):
                fpart[k, h, q + i] = fpart[k, h, q + i] + val[:, i * sr:(i + 1) * sr]
            local.append(send(fpart.at[k, h, q + 1 - core], drecv.at[k, h, s], ds_, dr, h, s, s, mr, partner))
        return local

    def fwd_pass(k, h, local):
        copies = []
        for s, other in zip(range(nch - 1, -1, -1), local):
            q = chip_at(s) * 2 + core
            other.wait_recv()
            part = fpart[k, h, q] + drecv[k, h, s]
            if s:
                col_pack(fsend.at[k, h, s], part)
                copies.append(send(fsend.at[k, h, s], frecv.at[k, h, s], fs, fr, h, s, s, mr, q))
            else:
                ray[k + 1, h] = part
        return copies

    def fwd_sum(k, h, copies):
        total = ray[k + 1, h]
        for i, copy in enumerate(copies):
            copy.wait_recv()
            total = total + col_unpack(frecv.at[k, h, nch - 1 - i], hz)
        return total

    def flip(first, last):
        @pl.loop(first, last)
        def _(d):
            for j in range(sv // LANE):
                cols = slice(j * LANE, (j + 1) * LANE)
                both = jnp.concatenate([vfull[0, d, :, cols], vfull[1, d, :, cols]], axis=0)
                vrow[block(d * sv + j * LANE, LANE), :] = both.T

    alphas = [[None, None] for _ in range(ITERS)]
    betas = [[None, None] for _ in range(ITERS + 1)]
    run = {}

    def update_dir(k):
        alpha = merge(*alphas[k])
        inv_alpha = 1.0 / alpha
        if k == 0:
            run["rho_bar"] = alpha
            sdir[...] = vrow[...] * inv_alpha
        else:
            theta = run["sine"] * alpha
            run["rho_bar"] = -run["cosine"] * alpha
            sdir[...] = vrow[...] * inv_alpha - (theta / run["rho"]) * sdir[...]

    def update_sol(k):
        beta = merge(*betas[k + 1])
        rho_bar = run["rho_bar"]
        rho = jnp.sqrt(rho_bar * rho_bar + beta * beta)
        run["rho"] = rho
        run["cosine"] = rho_bar / rho
        run["sine"] = beta / rho
        phi = run["cosine"] * run["phi_bar"]
        run["phi_bar"] = run["sine"] * run["phi_bar"]
        if k + 1 == ITERS:
            res[0:8] = jnp.broadcast_to(phi / rho, (8, z))
            res[8:16] = jnp.broadcast_to(run["phi_bar"], (8, z))
            return
        step = (phi / rho) * sdir[...]
        sol[...] = step if k == 0 else sol[...] + step

    def half(h):
        beta_of = None
        for k in range(ITERS):
            back_start(k, h)
            if k == 0 and h == 0:
                build_ba(mr)
            yield
            back_relay(k, h)
            if k == 0 and h == 0:
                build_ba(early)
            yield
            total = back_sum(k, h)
            if k:
                betas[k][h] = root(beta_of)
            elif not h:
                run["phi_bar"] = root(first_norm)
                betas[0] = [run["phi_bar"], run["phi_bar"]]
            beta = betas[k][h]
            raw = total * wide(column(1.0 / beta, h), sv)
            if k:
                raw = raw - wide(column(beta / alphas[k - 1][h], h), sv) * vox[k - 1, h]
            vox[k, h] = raw
            col_pack(vgat.at[k, h, mr], raw)
            vox_send(k, h)
            alpha_of = share_z(row_squares(raw), 2 * k + 1, h)
            vox_take(k, h, mr)
            fwd_grow(k, h, mr, True)
            if k == 0 and h == 0:
                build_ba(cross)
                build_ba(late)
            if k and h:
                update_sol(k - 1)
            yield
            vox_early(k, h)
            fwd_grow(k, h, early, False)
            yield
            passed(k, h, cross, 0, mate).wait_recv()
            vox_take(k, h, cross)
            fwd_grow(k, h, cross, False)
            yield
            passed(k, h, late, 0, mate).wait_recv()
            vox_take(k, h, late)
            local = fwd_send(k, h)
            alpha_of = share_c(alpha_of(), 2 * k + 1, h)
            yield
            copies = fwd_pass(k, h, local)
            if h:
                flip(0, nr)
            yield
            total = fwd_sum(k, h, copies)
            alpha = root(alpha_of)
            alphas[k][h] = alpha
            raw = total * wide(column(1.0 / alpha, h), sr)
            raw = raw - wide(column(alpha / beta, h), sr) * ray[k, h]
            n = 2 * k + 2
            if k + 1 == ITERS:
                beta_of = share_all(row_squares(raw), h)
                if h:
                    update_dir(k)
                yield
                betas[k + 1][h] = root(beta_of)
                return
            ray[k + 1, h] = raw
            own = yb.at[k + 1, h, mc]
            own[...] = raw.astype(jnp.bfloat16)
            across = [send(own, own, gs, gr, h, 0, 0, mr, partner)]
            for s in range(nch - 1, 0, -1):
                across.append(send(own, own, gs, gr, h, s, s, mr, chip_at(s) * 2 + core))
            beta_of = share_c(row_squares(raw), n, h)
            if h:
                update_dir(k)
            yield
            across[0].wait_recv()
            back_grow(k + 1, h, chip * 2, True)
            yield
            hand = []
            for s in range(nch - 1, 0, -1):
                across[nch - s].wait_recv()
                origin = chip_at(s) * 2 + core
                given = yb.at[k + 1, h, origin]
                hand.append(send(given, given, hs, hr, h, s, s, mr, partner))
            beta_of = share_z(beta_of(), n, h)
            yield
            for s in range(nch - 1, 0, -1):
                hand[nch - 1 - s].wait_recv()
                if s > 1:
                    back_grow(k + 1, h, chip_at(s) * 2, False)

    def build_fa(dest):
        wide_by = sv // tile

        @pl.loop(0, tr)
        def _(i):
            for j in range(wide_by):
                fa[block(i * tile, tile), block(dest * sv + j * tile, tile)] = pick(i, dest * wide_by + j)

    def build_ba(origin):
        wide_by = sv // tile

        @pl.loop(0, wide_by)
        def _(j):
            for i in range(tr):
                ba[block(origin * sv + j * tile, tile), i * tile:(i + 1) * tile] = pick(i, origin * wide_by + j).T

    place = jnp.broadcast_to(place_of[...], (LANE, slots)).T
    slot_of = lax.broadcasted_iota(jnp.int32, (slots, LANE), 0)
    for i in range(inv.shape[0]):
        spot = lax.broadcasted_iota(jnp.int32, (slots, LANE), 1) + i * LANE
        inv_row[i:i + 1, :] = jnp.min(jnp.where(place == spot, slot_of, slots), axis=0, keepdims=True)
    move = pltpu.make_async_copy(inv_row, inv, io.at[1])
    move.start()
    tiles[slots] = jnp.zeros((tile, tile), tiles.dtype)
    load_sino.wait()
    total = squares(sino[...])
    for i in range(tr):
        y0[:, i * tile:(i + 1) * tile] = sino[i * tile:(i + 1) * tile, :].T.astype(jnp.bfloat16)
    own = sino[block(mc * sr, sr), :].T
    ray[0, 0] = own[:hz]
    ray[0, 1] = own[hz:]
    move.wait()
    for load in load_tiles:
        load.wait()

    pl.semaphore_wait(barrier, nr * nc - 1)
    first_norm = share_z(total, 0, 0)
    halves = [half(0), half(1)]
    for h in ORDER:
        next(halves[h], None)
    update_sol(ITERS - 1)
    for key in list(pending):
        settle(key)

    @pl.when(inner)
    def _():
        for h in range(2):
            passed(0, h, mr, 2, far).wait_send()
            passed(0, h, far, 3, mate).wait_send()


def finish_kernel(x, d, scale, out, last, val, sems):
    parts = sems.shape[0]
    n = x.shape[0] // parts
    last[...] = scale[8:9, :]
    stores = []
    for i in range(parts):
        rows = pl.ds(i * n, n)
        val[rows, :] = x[rows, :] + scale[0:1, :] * d[rows, :]
        stores.append(pltpu.make_async_copy(val.at[rows], out.at[rows], sems.at[i]))
        stores[i].start()
    for store in stores:
        store.wait()


def body(nr, nc, tile_values, tile_rows, tile_cols, tile_count, sinogram):
    values = tile_values[0, 0]
    slots, tile = values.shape[0], values.shape[1]
    mb, z = sinogram.shape
    nb = TC * tile
    tr = mb // tile
    sv, sr = nb // nr, mb // nc
    if nr != 4 or nc != 8 or sr % LANE or sv % LANE or z != LANE:
        return body_rows(nr, nc, tile_values, tile_rows, tile_cols, tile_count, sinogram)
    ids = jnp.arange(slots, dtype=jnp.int32)[None, :]
    place = jnp.where(ids < tile_count, tile_rows[0] * TC + tile_cols[0], -1)
    nch, hz = nc // 2, z // 2
    f32, bf16, i16 = jnp.float32, jnp.bfloat16, jnp.int16
    dma, vmem_of = pltpu.SemaphoreType.DMA, pltpu.VMEM
    vmem = pl.BlockSpec(memory_space=pltpu.VMEM)
    hbm = pl.BlockSpec(memory_space=pltpu.HBM)
    pb, pf = sv // LANE * hz + PAD, sr // LANE * hz + PAD
    norms = 2 * ITERS + 1
    spots = tr * TC // LANE
    scratch = [
        vmem_of((slots + 1, tile, tile), bf16), vmem_of((mb, z), f32),
        vmem_of((spots, LANE), jnp.int32), pltpu.SMEM((spots, LANE), jnp.int32),
        vmem_of((mb, nb), bf16), vmem_of((nb, mb), bf16), vmem_of((z, mb), bf16),
        vmem_of((ITERS, 2, nc, hz, sr), bf16), vmem_of((2, nr, hz, sv), f32),
        vmem_of((ITERS, 2, nc, hz, sr), f32), vmem_of((ITERS, 2, nch, hz, sr), f32),
        vmem_of((2, nr, hz, sv), bf16), vmem_of((2, nr, hz, sv), f32),
        vmem_of((ITERS + 1, 2, hz, sr), f32), vmem_of((ITERS, 2, hz, sv), f32), vmem_of((2, hz, sv), f32),
        vmem_of((nb, z), f32),
        vmem_of((ITERS, 2, nr, pb, LANE), i16), vmem_of((ITERS, 2, nr, pb, LANE), i16),
        vmem_of((ITERS, 2, nr, pb, LANE), i16),
        vmem_of((ITERS, 2, nch, pf, LANE), i16), vmem_of((ITERS, 2, nch, pf, LANE), i16),
        vmem_of((norms, 2, nr, 8, z), f32), vmem_of((norms, 2, nc, 8, z), f32),
        vmem_of((2, nr * nc, 1, z), f32),
    ] + [dma((2, nr))] * 4 + [dma((2, nch))] * 8 + [dma((2, 2))] * 4 + [dma((2,))] * 2 + [dma((6,))]
    part = jax.ShapeDtypeStruct((nb, z), f32)
    sol, step, scale = pl.pallas_call(
        functools.partial(kernel, nr, nc),
        out_shape=(part, part, jax.ShapeDtypeStruct((16, z), f32)),
        in_specs=[vmem, hbm, hbm],
        out_specs=(vmem, vmem, vmem),
        scratch_shapes=scratch,
        compiler_params=pltpu.CompilerParams(
            collective_id=0, has_side_effects=True, vmem_limit_bytes=GRANT),
    )(place, values, sinogram)
    sol, last = pl.pallas_call(
        finish_kernel,
        out_shape=(part, jax.ShapeDtypeStruct((1, z), f32)),
        in_specs=[vmem, vmem, vmem],
        out_specs=(hbm, vmem),
        scratch_shapes=[vmem_of((nb, z), f32), dma((4,))],
        compiler_params=pltpu.CompilerParams(vmem_limit_bytes=8 * 1024 * 1024),
    )(sol, step, scale)
    return sol, last[0]


def solution(mesh):
    nr, nc = mesh.shape["row"], mesh.shape["col"]
    in_specs = (
        P("row", "col", None, None, None),
        P("row", "col", None),
        P("row", "col", None),
        P("row", "col"),
        P("row", None),
    )
    return jax.shard_map(
        functools.partial(body, nr, nc), mesh=mesh, in_specs=in_specs,
        out_specs=(P("col", None), P()), check_vma=False)
```
